128 devices in a mesh: cp: 64 (over x, z, y), hd: 2 (over core).
Axes of the slice: x: 4, y: 4, z: 4, core: 2. Of those that a mesh axis runs over, the one named last changes fastest.
Arguments:
- queries: bfloat16 [12288, 4096], P('cp', 'hd'), may hold values from -48 to 48
- keys: bfloat16 [12288, 1024], P('cp', 'hd'), may hold values from -48 to 48
- values: bfloat16 [12288, 1024], P('cp', 'hd'), may hold values from -6 to 6
- span_table: int32 [128], replicated, may hold values from 0 to 127, as said below
- doc_ids: int32 [12288], replicated, may hold values from 0 to 7, never falling along the last dimension, each value on 1 to 3072 neighbouring positions
- out_weight: bfloat16 [4096, 4096], P('hd'), may hold values from -0.09375 to 0.09375
Outputs:
- mixed: bfloat16 [12288, 4096], P(('cp', 'hd'))
The draws below stay inside these ranges and needn't reach their ends.
Inputs may be any that keep to these rules, and one draw needn't show every extreme that they name: `span_table`: slots 2 j and 2 j + 1 hold two spans c and 127 - c, and every span is held once.
All inputs are finite; a program needn't handle non-finite values.
Results may differ from the reference program's by a relative error of at most 0.0095.
Values may be sent and summed in bfloat16 or wider, within the bound.
A program may use at most 128 MiB of HBM per device.

```python
import math
import jax
import jax.numpy as jnp
import numpy as np
from jax import lax

D = 4096
QUERY_HEADS = 32
KEY_VALUE_HEADS = 8
HEAD_WIDTH = 128
SPAN_TOKENS = 96
DOCS = 8
SPANS = 128
SEQUENCE_TOKENS = 12288


def paired_table(key):
    pairs = jax.random.permutation(jax.random.fold_in(key, 11), SPANS // 2).astype(jnp.int32)
    flips = jax.random.randint(jax.random.fold_in(key, 12), (SPANS // 2,), 0, 2)
    upper = (SPANS - 1 - pairs).astype(jnp.int32)
    first = jnp.where(flips == 1, upper, pairs)
    second = jnp.where(flips == 1, pairs, upper)
    return jnp.stack([first, second], axis=1).reshape(SPANS).astype(jnp.int32)


def draw_span_table(key, part):
    return paired_table(key)


def drawn_pair(key):
    drawn_key_rows = jnp.clip(jax.random.normal(jax.random.fold_in(key, 21), (SEQUENCE_TOKENS, KEY_VALUE_HEADS * HEAD_WIDTH), jnp.float32), -6.0, 6.0)
    base_queries = jnp.clip(jax.random.normal(jax.random.fold_in(key, 22), (SEQUENCE_TOKENS, QUERY_HEADS * HEAD_WIDTH), jnp.float32), -6.0, 6.0)
    new_keys = drawn_key_rows
    new_queries = base_queries
    return (jnp.clip(new_queries, -48.0, 48.0), jnp.clip(new_keys, -48.0, 48.0))


def draw_queries(key, part):
    return drawn_pair(key)[0].astype(jnp.bfloat16)


def draw_keys(key, part):
    return drawn_pair(key)[1].astype(jnp.bfloat16)


def block_levels(rng, dims, shards, smallest, high):
    def one(dim, blocks):
        steps = jax.random.uniform(jax.random.fold_in(jax.random.fold_in(rng, 6), dim), (blocks,), jnp.float32, smallest / len(shards), high / len(shards))
        return jnp.repeat(jnp.exp(steps), dims[dim] // blocks).reshape((-1,) + (1,) * (len(dims) - dim - 1))

    gain = one(*shards[0])
    for cut in shards[1:]:
        gain = gain * one(*cut)
    return gain


def split_up(amount, total, bound, slope):
    portions = [(1 << 20) // math.isqrt(rank ** slope) + 1 for rank in range(2, amount + 1)]
    surplus, given = total - bound - (amount - 1), [1] * (amount - 1)
    while surplus > 0:
        movable = [i for i in range(amount - 1) if given[i] < bound]
        pool, left = sum([portions[i] for i in movable]), surplus
        for i in movable:
            extra = min(bound - given[i], max(1, left * portions[i] // pool), surplus)
            given[i] = given[i] + extra
            surplus = surplus - extra
    return np.array([bound] + given)


def ragged_sizes(own_key, count, total, limit, lean):
    if count == 2:
        one = jax.random.randint(own_key, (), max(1, total - limit), min(limit, total - 1) + 1)
        return jnp.stack([one, total - one])
    sizes = jnp.asarray(split_up(count, total, limit, lean), jnp.int32)
    twos = (count - 1) // 2
    source_of, taker = sizes[1:1 + 2 * twos:2], sizes[2:2 + 2 * twos:2]
    room = jnp.minimum(source_of - 1, limit - taker)
    moved = jax.random.randint(jax.random.fold_in(own_key, 1), (twos,), 0, 1 << 20) % (room + 1)
    sizes = sizes.at[1:1 + 2 * twos:2].set(source_of - moved).at[2:2 + 2 * twos:2].set(taker + moved)
    return sizes[jax.random.permutation(jax.random.fold_in(own_key, 2), count)]


def centred(key, dims, width, bound, cuts=(), kind=jnp.bfloat16):
    gain = block_levels(key, dims, cuts, -0.22, 0.18) if cuts else 1.0
    values = jax.random.normal(key, dims, jnp.float32) * width * gain
    return jnp.minimum(jnp.maximum(values, -bound), bound).astype(kind)


def setup_inputs(seed: int = 0) -> dict:
    seeds = jax.random.split(jax.random.key(seed), 7)
    return {
        "queries": draw_queries(jax.random.fold_in(seeds[6], 71), 0),
        "keys": draw_keys(jax.random.fold_in(seeds[6], 71), 0),
        "values": centred(seeds[2], (SEQUENCE_TOKENS, KEY_VALUE_HEADS * HEAD_WIDTH), 1.0, 6.0, ((0, 64), (1, 2))),
        "span_table": draw_span_table(jax.random.fold_in(seeds[6], 71), 0),
        "doc_ids": jnp.searchsorted(jnp.cumsum(ragged_sizes(seeds[4], DOCS, SEQUENCE_TOKENS, SEQUENCE_TOKENS // 4, 2)), jnp.arange(SEQUENCE_TOKENS), side="right").astype(jnp.int32),
        "out_weight": centred(seeds[5], (QUERY_HEADS * HEAD_WIDTH, D), (QUERY_HEADS * HEAD_WIDTH) ** -0.5, 0.09375, ((0, 2),)),
    }


def reference(queries, keys, values, span_table, doc_ids, out_weight):
    query_group = QUERY_HEADS // KEY_VALUE_HEADS
    scale = HEAD_WIDTH ** -0.5
    rows = jnp.arange(SEQUENCE_TOKENS, dtype=jnp.int32)
    positions = (span_table[rows // SPAN_TOKENS] * SPAN_TOKENS + rows % SPAN_TOKENS).astype(jnp.int32)
    documents = doc_ids[positions]
    key_head_rows = keys.reshape(SEQUENCE_TOKENS, KEY_VALUE_HEADS, HEAD_WIDTH).astype(jnp.float32)
    value_head_rows = values.reshape(SEQUENCE_TOKENS, KEY_VALUE_HEADS, HEAD_WIDTH).astype(jnp.float32)

    def block(index):
        first = (index * SPAN_TOKENS).astype(jnp.int32)
        query_matrix = lax.dynamic_slice_in_dim(queries, first, SPAN_TOKENS, 0)
        query_matrix = query_matrix.reshape(SPAN_TOKENS, KEY_VALUE_HEADS, query_group, HEAD_WIDTH).astype(jnp.float32)
        query_pos = lax.dynamic_slice_in_dim(positions, first, SPAN_TOKENS, 0)
        query_doc = lax.dynamic_slice_in_dim(documents, first, SPAN_TOKENS, 0)
        visible = (positions[None, :] <= query_pos[:, None]) & (documents[None, :] == query_doc[:, None])
        scores = jnp.einsum("qkgd,nkd->kgqn", query_matrix, key_head_rows) * scale
        scores = jnp.where(visible, scores, -1e30)
        best = jnp.max(scores, axis=-1, keepdims=True)
        weights = jnp.where(visible, jnp.exp(scores - best), 0.0)
        denom = jnp.sum(weights, axis=-1)
        rounded = lax.optimization_barrier(weights.astype(jnp.bfloat16)).astype(jnp.float32)
        numer = jnp.einsum("kgqn,nkd->kgqd", rounded, value_head_rows)
        result = numer / denom[..., None]
        return result.transpose(2, 0, 1, 3).reshape(SPAN_TOKENS, QUERY_HEADS * HEAD_WIDTH).astype(jnp.bfloat16)

    attn = lax.map(block, jnp.arange(SEQUENCE_TOKENS // SPAN_TOKENS, dtype=jnp.int32)).reshape(SEQUENCE_TOKENS, QUERY_HEADS * HEAD_WIDTH)
    return jnp.dot(attn, out_weight, preferred_element_type=jnp.float32).astype(jnp.bfloat16)
```

```python
import functools
import math

import jax
import jax.numpy as jnp
from jax import lax
from jax.experimental import pallas as pl
from jax.experimental.pallas import tpu as pltpu
from jax.sharding import PartitionSpec as P

WIDTH = 128
SPAN = 96
GROUP = 4
ROWS = GROUP * SPAN
PIECES = 8
DOCS = 8
BACK = 32
STEP = 8
KEYS = STEP * SPAN
STEPS = BACK // STEP
NEG = -1e30
MESH = pl.DeviceIdType.MESH
FACTOR = WIDTH ** -0.5 * math.log2(math.e)
ARRIVAL = (0, 1, 3, 4, 2, 5, 7, 6)
EARLY = (0, 1, 3, 4, 2)
RETURN = (6, 5, 7, 2, 4, 1, 3, 0)


def kernel(
    span_ref, span_row_ref, doc_ref, q_hbm, k_hbm, v_hbm, w_hbm, out_ref,
    q_in, k_in, v_in, kv, q_buf, o_buf, attn, w_vmem, scores, own_acc, own_top, penalty, table,
    outgoing, incoming, kept, index,
    load_sem, local_sem, w_sem, table_sem,
    su, sq, ru, rq, s_own, s_far, s_half, s_z, rx, rz, sd, rd, so, ro, xs, xr,
):
    me = lax.axis_index("cp")
    hd = lax.axis_index("hd")
    other = 1 - hd
    x, z, y = me // 16, (me // 4) % 4, me % 4
    home = (z // 2) == hd
    zp = z + 1 - 2 * (z % 2)

    def chip(xx, zz, yy):
        return xx * 16 + zz * 4 + yy

    right, left, across = chip((x + 1) % 4, z, y), chip((x + 3) % 4, z, y), chip(x, zp, y)

    def source(xo, zo, i):
        return chip(xo, 3 - zo if i >= 4 else zo, (y + i % 4) % 4)

    def remote(src, dst, send, recv, cp, core):
        return pltpu.make_async_remote_copy(
            src_ref=src, dst_ref=dst, send_sem=send, recv_sem=recv,
            device_id={"cp": cp, "hd": core}, device_id_type=MESH,
        )

    def landed(dst, sem):
        remote(dst, dst, sd.at[0], sem, me, other).wait_recv()

    def go(copy):
        copy.start()

    def sent(copy):
        copy.wait_send()

    my_rows = pl.ds(pl.multiple_of(hd * SPAN, SPAN), SPAN)
    my_head = pl.ds(pl.multiple_of(y * WIDTH, WIDTH), WIDTH)
    my_queries = pl.ds(pl.multiple_of(y * GROUP * WIDTH, GROUP * WIDTH), GROUP * WIDTH)

    loads = [
        pltpu.make_async_copy(k_hbm, k_in, load_sem.at[0]),
        pltpu.make_async_copy(v_hbm, v_in, load_sem.at[1]),
        pltpu.make_async_copy(q_hbm, q_in, load_sem.at[2]),
    ]
    locals_ = [
        pltpu.make_async_copy(k_hbm.at[my_rows, my_head], kv.at[2 * me + hd, 0], ru.at[0, 0]),
        pltpu.make_async_copy(v_hbm.at[my_rows, my_head], kv.at[2 * me + hd, 1], ru.at[0, 1]),
        pltpu.make_async_copy(q_hbm.at[my_rows, my_queries], q_buf.at[0], rq.at[0]),
    ]
    w_load = pltpu.make_async_copy(w_hbm, w_vmem, w_sem)
    for load in loads:
        load.start()

    barrier = pltpu.get_barrier_semaphore()

    def greet(cp, core):
        pl.semaphore_signal(barrier, inc=1, device_id={"cp": cp, "hd": core}, device_id_type=MESH)

    for i in range(PIECES):
        for core in (hd, other):
            if i or core is other:
                greet(source(x, z, i), core)
    for target in (right, left, across):
        greet(target, hd)

    spans = jnp.broadcast_to(span_row_ref[...].astype(jnp.float32), (128, 128)).T
    held_by = lax.broadcasted_iota(jnp.int32, (128, 128), 0).astype(jnp.float32)
    wanted = lax.broadcasted_iota(jnp.int32, (128, 128), 1).astype(jnp.float32)
    table[0:1, :] = jnp.max(jnp.where(spans == wanted, held_by, 0.0), axis=0, keepdims=True).astype(jnp.int32)
    docs = doc_ref[...]
    lane = lax.broadcasted_iota(jnp.int32, (1, 128), 1)
    starts = jnp.zeros((1, 128), jnp.float32)
    for d in range(1, DOCS):
        first = jnp.sum(jnp.where(docs < d, 1.0, 0.0), keepdims=True)
        starts = jnp.where(lane == d, first, starts)
    table[1:2, :] = starts.astype(jnp.int32)

    pl.semaphore_wait(barrier, 2 * PIECES + 2)

    tz = jnp.where(home, z, 3 - z)

    def scatter(act, what):
        for dj in (0, 1, 3, 2):
            j = (y + dj) % 4
            to = chip(x, tz, j)
            piece = jnp.where(home, 0, 4) + (4 - dj) % 4
            for rel, core in enumerate((hd, other)):
                rows = pl.ds(pl.multiple_of(core * SPAN, SPAN), SPAN)

                def one():
                    if what == "kv":
                        columns = pl.ds(pl.multiple_of(j * WIDTH, WIDTH), WIDTH)
                        for v, staged in enumerate((k_in, v_in)):
                            act(remote(staged.at[rows, columns], kv.at[2 * me + core, v],
                                       su.at[dj, rel, v], ru.at[piece, v], to, core))
                    else:
                        columns = pl.ds(pl.multiple_of(j * GROUP * WIDTH, GROUP * WIDTH), GROUP * WIDTH)
                        act(remote(q_in.at[rows, columns], q_buf.at[piece],
                                   sq.at[dj, rel], rq.at[piece], to, core))

                if dj == 0 and rel == 0:
                    pl.when(jnp.logical_not(home))(one)
                else:
                    one()

    @pl.when(home)
    def _():
        for copy in locals_:
            copy.start()

    loads[0].wait()
    loads[1].wait()
    scatter(go, "kv")
    loads[2].wait()
    scatter(go, "q")
    w_load.start()
    table_copy = pltpu.make_async_copy(table, index, table_sem)

    def piece_of(xo, zo, i):
        return kv.at[2 * source(xo, zo, i) + hd]

    def share(act, xo, zo, i):
        s = source(xo, zo, i)
        part = kv.at[2 * s + hd]
        act(remote(part, part, sd.at[s], rd.at[s], me, other))

    x_left, x_right, x_far = (x + 3) % 4, (x + 1) % 4, (x + 2) % 4

    def relay(act, between=None):
        waiting = act is go
        for i in ARRIVAL:
            part = piece_of(x, z, i)
            if waiting:
                landed(part.at[0], ru.at[i, 0])
                landed(part.at[1], ru.at[i, 1])
            act(remote(part, part, s_own.at[i, 0], rx.at[0, 0, i], right, hd))
            act(remote(part, part, s_own.at[i, 1], rx.at[1, 0, i], left, hd))
            act(remote(part, part, s_own.at[i, 2], rz.at[0, i], across, hd))
            share(act, x, z, i)
        for i in ARRIVAL:
            if i in EARLY:
                part = piece_of(x, zp, i)
                if waiting:
                    landed(part, rz.at[0, i])
                act(remote(part, part, s_far.at[i, 0], rx.at[0, 1, i], right, hd))
                act(remote(part, part, s_far.at[i, 1], rx.at[1, 1, i], left, hd))
                share(act, x, zp, i)
        for zrel, zo in ((0, z), (1, zp)):
            for i in ARRIVAL:
                if zrel and i not in EARLY:
                    continue
                for side, xo, onward, half in ((0, x_left, right, 0), (1, x_right, left, 1)):
                    part = piece_of(xo, zo, i)
                    if waiting:
                        landed(part, rx.at[side, zrel, i])
                    act(remote(part.at[half], part.at[half], s_half.at[side, zrel, i],
                               rx.at[2 + side, zrel, i], onward, hd))
                    if i not in EARLY:
                        act(remote(part, part, s_z.at[side, i], rz.at[1 + side, i], across, hd))
                    share(act, xo, zo, i)
        if waiting:
            between()
        for zrel, zo in ((0, z), (1, zp)):
            for i in ARRIVAL:
                if zrel and i not in EARLY:
                    continue
                part = piece_of(x_far, zo, i)
                if waiting:
                    landed(part.at[0], rx.at[2, zrel, i])
                    landed(part.at[1], rx.at[3, zrel, i])
                if i not in EARLY:
                    act(remote(part, part, s_z.at[2, i], rz.at[3, i], across, hd))
                share(act, x_far, zo, i)
        for n, xo in enumerate((x, x_left, x_right, x_far)):
            for i in ARRIVAL:
                if i not in EARLY:
                    if waiting:
                        landed(piece_of(xo, zp, i), rz.at[n, i])
                    share(act, xo, zp, i)

    ones = jnp.ones((KEYS, WIDTH), jnp.bfloat16)

    def slot_of(i):
        return 2 * chip(x, jnp.where(i >= 4, 3 - z, z), (y + i % 4) % 4) + hd

    def queries_of(i):
        whole = q_buf[i]
        return jnp.concatenate([whole[:, g * WIDTH:(g + 1) * WIDTH] for g in range(GROUP)], axis=0)

    def score(q, keys):
        return lax.dot_general(q, keys, (((1,), (1,)), ((), ())), preferred_element_type=jnp.float32)

    def own(i, carry):
        landed(q_buf.at[i], rq.at[i])
        slot = slot_of(i)
        begin = span_ref[slot] * SPAN
        row = lax.broadcasted_iota(jnp.int32, (SPAN, WIDTH), 0)
        low = jnp.zeros((SPAN, WIDTH), jnp.int32)
        for d in range(1, DOCS):
            start = index[1, d]
            low = jnp.maximum(low, jnp.where(start <= begin + row, start, 0))
        low = low - begin
        penalty[i] = jnp.where(low < 0, 0.0, -NEG)
        key = lax.broadcasted_iota(jnp.int32, (SPAN, WIDTH), 1)
        bias = jnp.where((key >= low) & (key <= row), 0.0, NEG)[:, :SPAN]
        s = score(queries_of(i), kv[slot, 0]) + jnp.concatenate([bias] * GROUP, axis=0)
        top = jnp.max(s, axis=1, keepdims=True)
        weights = jnp.exp2(s * FACTOR - top * FACTOR).astype(jnp.bfloat16)
        own_top[i] = jnp.broadcast_to(top, (ROWS, WIDTH))
        values = jnp.concatenate([kv[slot, 1], ones[:SPAN]], axis=1)
        own_acc[i] = jnp.dot(weights, values, preferred_element_type=jnp.float32)
        return carry

    def own_blocks():
        lax.fori_loop(0, PIECES, own, 0)

    table_copy.start()
    table_copy.wait()
    relay(go, own_blocks)

    def shared(s, carry):
        landed(kv.at[2 * s + other], rd.at[s])
        return carry

    lax.fori_loop(0, 64, shared, 0)

    where_key = lax.broadcasted_iota(jnp.int32, (1, KEYS), 1)
    where_key = where_key - 2 * SPAN * (where_key // SPAN)

    def give_back(act, i):
        to = chip(x, jnp.where(i >= 4, 3 - z, z), (y + i % 4) % 4)
        act(remote(o_buf.at[i], attn.at[my_rows, my_queries], so.at[i], ro.at[hd * 4 + y], to, z // 2))

    def slot_at(place):
        return jnp.clip(index[0, jnp.clip(place, 0, 127)], 0, 127)

    def attend(n, carry):
        i = jnp.int32(0)
        for k, piece in enumerate(RETURN):
            i = jnp.where(n == k, piece, i)
        slot = slot_of(i)
        c = span_ref[slot]
        begin = c * SPAN
        low = jnp.int32(0)
        for d in range(1, DOCS):
            start = index[1, d]
            low = jnp.maximum(low, jnp.where(start <= begin, start, 0))
        q = queries_of(i)
        peak = jnp.full((ROWS, WIDTH), NEG, jnp.float32)
        for j in range(STEPS):
            slots = [slot_at(c - 1 - (STEP * j + t)) for t in range(STEP)]
            keys = jnp.concatenate([kv[s, 0] for s in slots], axis=0)
            bias = jnp.where(where_key >= low - SPAN * (c - 1 - STEP * j), 0.0, NEG)
            for h in range(KEYS // 256):
                cut = slice(h * 256, (h + 1) * 256)
                part = score(q, keys[cut]) + bias[:, cut]
                scores[:, j * KEYS + h * 256:j * KEYS + (h + 1) * 256] = part
                peak = jnp.maximum(peak, jnp.maximum(part[:, :WIDTH], part[:, WIDTH:]))
        fence = jnp.concatenate([penalty[i]] * GROUP, axis=0)
        mine = own_top[i]
        top = jnp.maximum(jnp.max(peak, axis=1, keepdims=True) - fence, mine)
        fade = jnp.exp2((mine - top) * FACTOR)
        acc = own_acc[i] * jnp.concatenate([fade, fade], axis=1)
        shift = top * FACTOR + fence
        shift = jnp.concatenate([shift] * (KEYS // WIDTH), axis=1)
        for j in range(STEPS):
            slots = [slot_at(c - 1 - (STEP * j + t)) for t in range(STEP)]
            values = jnp.concatenate([kv[s, 1] for s in slots], axis=0)
            values = jnp.concatenate([values, ones], axis=1)
            weights = jnp.exp2(scores[:, j * KEYS:(j + 1) * KEYS] * FACTOR - shift).astype(jnp.bfloat16)
            acc = acc + jnp.dot(weights, values, preferred_element_type=jnp.float32)
        result = (acc[:, :WIDTH] / acc[:, WIDTH:]).astype(jnp.bfloat16)
        for g in range(GROUP):
            o_buf[i, :, g * WIDTH:(g + 1) * WIDTH] = result[g * SPAN:(g + 1) * SPAN]
        local = home & (i == 0)

        @pl.when(local)
        def _():
            attn[my_rows, my_queries] = o_buf[0]

        @pl.when(jnp.logical_not(local))
        def _():
            give_back(go, i)

        return carry

    lax.fori_loop(0, PIECES, attend, 0)

    for k in range(2):
        for j in range(4):
            @pl.when(jnp.logical_not(home & (hd == k) & (y == j)))
            def _():
                landed(attn.at[pl.ds(k * SPAN, SPAN), pl.ds(j * GROUP * WIDTH, GROUP * WIDTH)], ro.at[k * 4 + j])

    w_load.wait()
    count, width = outgoing.shape[0], outgoing.shape[2]

    def hand_over(n):
        return remote(outgoing.at[n], incoming.at[n], xs.at[n], xr.at[n], me, other)

    @pl.loop(0, count)
    def _(n):
        columns = pl.ds(pl.multiple_of(n * width, width), width)
        product = jnp.dot(attn[...], w_vmem[:, columns], preferred_element_type=jnp.float32)
        upper, lower = product[:SPAN], product[SPAN:]
        first = hd == 0
        outgoing[n] = jnp.where(first, lower, upper).astype(jnp.bfloat16)
        kept[n] = jnp.where(first, upper, lower)
        hand_over(n).start()

    for n in range(count):
        hand_over(n).wait_recv()
        out_ref[:, n * width:(n + 1) * width] = (kept[n] + incoming[n].astype(jnp.float32)).astype(jnp.bfloat16)

    for n in range(count):
        hand_over(n).wait_send()
    scatter(sent, "kv")
    scatter(sent, "q")
    relay(sent)
    for i in range(PIECES):
        if i:
            give_back(sent, jnp.int32(i))
        else:
            pl.when(jnp.logical_not(home))(lambda: give_back(sent, jnp.int32(0)))


def local(queries, keys, values, span_table, doc_ids, out_weight):
    model = out_weight.shape[1]
    count = 8
    vmem, hbm = pltpu.VMEM, pl.ANY
    spec = lambda space: pl.BlockSpec(memory_space=space)
    dma = pltpu.SemaphoreType.DMA
    f32, bf16, i32 = jnp.float32, jnp.bfloat16, jnp.int32
    return pl.pallas_call(
        kernel,
        out_shape=jax.ShapeDtypeStruct((SPAN, model), bf16),
        in_specs=[spec(pltpu.SMEM), spec(vmem), spec(vmem), spec(hbm), spec(hbm), spec(hbm), spec(hbm)],
        out_specs=spec(vmem),
        scratch_shapes=[
            vmem(queries.shape, bf16),
            vmem(keys.shape, bf16),
            vmem(values.shape, bf16),
            vmem((128, 2, SPAN, WIDTH), bf16),
            vmem((PIECES, SPAN, GROUP * WIDTH), bf16),
            vmem((PIECES, SPAN, GROUP * WIDTH), bf16),
            vmem(queries.shape, bf16),
            vmem(out_weight.shape, bf16),
            vmem((ROWS, BACK * SPAN), f32),
            vmem((PIECES, ROWS, 2 * WIDTH), f32),
            vmem((PIECES, ROWS, WIDTH), f32),
            vmem((PIECES, SPAN, WIDTH), f32),
            vmem((8, 128), i32),
            vmem((count, SPAN, model // count), bf16),
            vmem((count, SPAN, model // count), bf16),
            vmem((count, SPAN, model // count), f32),
            pltpu.SMEM((8, 128), i32),
            dma((3,)), dma((3,)), dma, dma,
            dma((4, 2, 2)), dma((4, 2)), dma((PIECES, 2)), dma((PIECES,)),
            dma((PIECES, 3)), dma((PIECES, 2)), dma((2, 2, PIECES)), dma((3, PIECES)),
            dma((4, 2, PIECES)), dma((4, PIECES)), dma((64,)), dma((64,)),
            dma((PIECES,)), dma((PIECES,)), dma((count,)), dma((count,)),
        ],
        compiler_params=pltpu.CompilerParams(
            collective_id=0, has_side_effects=True, vmem_limit_bytes=60 * 2 ** 20,
        ),
    )(span_table, span_table.reshape(1, 128), doc_ids.reshape(-1, 128), queries, keys, values, out_weight)


def solution(mesh):
    return jax.shard_map(
        local,
        mesh=mesh,
        in_specs=(P("cp", "hd"), P("cp", "hd"), P("cp", "hd"), P(), P(), P("hd", None)),
        out_specs=P(("cp", "hd"), None),
        check_vma=False,
    )
```

```python
import functools
import math

import jax
import jax.numpy as jnp
from jax import lax
from jax.experimental import pallas as pl
from jax.experimental.pallas import tpu as pltpu
from jax.sharding import PartitionSpec as P

WIDTH = 128
SPAN = 96
GROUP = 4
ROWS = GROUP * SPAN
PIECES = 8
DOCS = 8
BACK = 32
STEP = 8
KEYS = STEP * SPAN
BLOCKS = BACK * SPAN // 256
NEG = -1e30
MESH = pl.DeviceIdType.MESH
FACTOR = WIDTH ** -0.5 * math.log2(math.e)
ARRIVAL = (0, 1, 3, 4, 2, 5, 7, 6)
EARLY = (0, 1, 3, 4)
SPLIT = 2
RETURN = (6, 5, 7, 2, 4, 1, 3, 0)


def kernel(
    span_hbm, span_row_hbm, doc_hbm, q_hbm, k_hbm, v_hbm, w_hbm, out_ref,
    q_in, k_in, v_in, kv, q_buf, o_buf, attn, w_vmem, scores0, scores1, shift0, shift1, fade0, fade1, peak, place_of, own_acc, own_top, penalty, table,
    outgoing, incoming, kept, result_of, span_row_ref, doc_ref, span_ref, index,
    load_sem, small_sem, w_sem, table_sem, out_sem,
    su, sq, ru, rq, s_own, s_far, s_half, s_z, rx, rz, sd, rd, so, ro, xs, xr,
):
    me = lax.axis_index("cp")
    hd = lax.axis_index("hd")
    other = 1 - hd
    x, z, y = me // 16, (me // 4) % 4, me % 4
    home = (z // 2) == hd
    zp = z + 1 - 2 * (z % 2)

    def chip(xx, zz, yy):
        return xx * 16 + zz * 4 + yy

    right, left, across = chip((x + 1) % 4, z, y), chip((x + 3) % 4, z, y), chip(x, zp, y)

    def source(xo, zo, i):
        return chip(xo, 3 - zo if i >= 4 else zo, (y + i % 4) % 4)

    def remote(src, dst, send, recv, cp, core):
        return pltpu.make_async_remote_copy(
            src_ref=src, dst_ref=dst, send_sem=send, recv_sem=recv,
            device_id={"cp": cp, "hd": core}, device_id_type=MESH,
        )

    def landed(dst, sem):
        remote(dst, dst, sd.at[0], sem, me, other).wait_recv()

    def go(copy):
        copy.start()

    def sent(copy):
        copy.wait_send()

    my_rows = pl.ds(pl.multiple_of(hd * SPAN, SPAN), SPAN)
    my_head = pl.ds(pl.multiple_of(y * WIDTH, WIDTH), WIDTH)
    my_queries = pl.ds(pl.multiple_of(y * GROUP * WIDTH, GROUP * WIDTH), GROUP * WIDTH)

    loads = [
        pltpu.make_async_copy(k_hbm, k_in, load_sem.at[0]),
        pltpu.make_async_copy(v_hbm, v_in, load_sem.at[1]),
        pltpu.make_async_copy(q_hbm, q_in, load_sem.at[2]),
    ]
    locals_ = [
        pltpu.make_async_copy(k_hbm.at[my_rows, my_head], kv.at[2 * me + hd, 0], ru.at[0, 0]),
        pltpu.make_async_copy(v_hbm.at[my_rows, my_head], kv.at[2 * me + hd, 1], ru.at[0, 1]),
        pltpu.make_async_copy(q_hbm.at[my_rows, my_queries], q_buf.at[0], rq.at[0]),
    ]
    w_load = pltpu.make_async_copy(w_hbm, w_vmem, w_sem)
    small = [
        pltpu.make_async_copy(span_row_hbm, span_row_ref, small_sem.at[0]),
        pltpu.make_async_copy(doc_hbm, doc_ref, small_sem.at[1]),
        pltpu.make_async_copy(span_hbm, span_ref, small_sem.at[2]),
    ]
    for load in loads + small:
        load.start()

    barrier = pltpu.get_barrier_semaphore()

    def greet(cp, core):
        pl.semaphore_signal(barrier, inc=1, device_id={"cp": cp, "hd": core}, device_id_type=MESH)

    for i in range(PIECES):
        for core in (hd, other):
            if i or core is other:
                greet(source(x, z, i), core)
    for target in (right, left, across):
        greet(target, hd)

    for load in small:
        load.wait()
    spans = jnp.broadcast_to(span_row_ref[...].astype(jnp.float32), (128, 128)).T
    held_by = lax.broadcasted_iota(jnp.int32, (128, 128), 0).astype(jnp.float32)
    wanted = lax.broadcasted_iota(jnp.int32, (128, 128), 1).astype(jnp.float32)
    table[0:1, :] = jnp.max(jnp.where(spans == wanted, held_by, 0.0), axis=0, keepdims=True).astype(jnp.int32)
    docs = doc_ref[...]
    lane = lax.broadcasted_iota(jnp.int32, (1, 128), 1)
    starts = jnp.zeros((1, 128), jnp.float32)
    for d in range(1, DOCS):
        first = jnp.sum(jnp.where(docs < d, 1.0, 0.0), keepdims=True)
        starts = jnp.where(lane == d, first, starts)
    table[1:2, :] = starts.astype(jnp.int32)

    pl.semaphore_wait(barrier, 2 * PIECES + 2)

    tz = jnp.where(home, z, 3 - z)

    def scatter(act, what):
        for dj in (0, 1, 3, 2):
            j = (y + dj) % 4
            to = chip(x, tz, j)
            piece = jnp.where(home, 0, 4) + (4 - dj) % 4
            for rel, core in enumerate((hd, other)):
                rows = pl.ds(pl.multiple_of(core * SPAN, SPAN), SPAN)

                def one():
                    if what == "kv":
                        columns = pl.ds(pl.multiple_of(j * WIDTH, WIDTH), WIDTH)
                        for v, staged in enumerate((k_in, v_in)):
                            act(remote(staged.at[rows, columns], kv.at[2 * me + core, v],
                                       su.at[dj, rel, v], ru.at[piece, v], to, core))
                    else:
                        columns = pl.ds(pl.multiple_of(j * GROUP * WIDTH, GROUP * WIDTH), GROUP * WIDTH)
                        act(remote(q_in.at[rows, columns], q_buf.at[piece],
                                   sq.at[dj, rel], rq.at[piece], to, core))

                if dj == 0 and rel == 0:
                    pl.when(jnp.logical_not(home))(one)
                else:
                    one()

    @pl.when(home)
    def _():
        for copy in locals_:
            copy.start()

    loads[0].wait()
    loads[1].wait()
    scatter(go, "kv")
    loads[2].wait()
    scatter(go, "q")
    w_load.start()
    table_copy = pltpu.make_async_copy(table, index, table_sem)

    def piece_of(xo, zo, i):
        return kv.at[2 * source(xo, zo, i) + hd]

    def share(act, xo, zo, i):
        s = source(xo, zo, i)
        part = kv.at[2 * s + hd]
        act(remote(part, part, sd.at[s], rd.at[s], me, other))

    x_left, x_right, x_far = (x + 3) % 4, (x + 1) % 4, (x + 2) % 4

    def if_early(i, fn):
        if i == SPLIT:
            pl.when(hd == 0)(fn)
        elif i in EARLY:
            fn()

    def if_late(i, fn):
        if i == SPLIT:
            pl.when(hd == 1)(fn)
        elif i not in EARLY:
            fn()

    def relay(act, between=None):
        waiting = act is go
        for i in ARRIVAL:
            part = piece_of(x, z, i)
            if waiting:
                landed(part.at[0], ru.at[i, 0])
                landed(part.at[1], ru.at[i, 1])
            act(remote(part, part, s_own.at[i, 0], rx.at[0, 0, i], right, hd))
            act(remote(part, part, s_own.at[i, 1], rx.at[1, 0, i], left, hd))
            act(remote(part, part, s_own.at[i, 2], rz.at[0, i], across, hd))
            share(act, x, z, i)

        def from_across(i):
            part = piece_of(x, zp, i)
            if waiting:
                landed(part, rz.at[0, i])
            act(remote(part, part, s_far.at[i, 0], rx.at[0, 1, i], right, hd))
            act(remote(part, part, s_far.at[i, 1], rx.at[1, 1, i], left, hd))
            share(act, x, zp, i)

        def from_side(i, zrel, zo):
            for side, xo, onward, half in ((0, x_left, right, 0), (1, x_right, left, 1)):
                part = piece_of(xo, zo, i)
                if waiting:
                    landed(part, rx.at[side, zrel, i])
                act(remote(part.at[half], part.at[half], s_half.at[side, zrel, i],
                           rx.at[2 + side, zrel, i], onward, hd))
                if not zrel:
                    if_late(i, lambda: act(remote(part, part, s_z.at[side, i], rz.at[1 + side, i], across, hd)))
                share(act, xo, zo, i)

        def from_far(i, zrel, zo):
            part = piece_of(x_far, zo, i)
            if waiting:
                landed(part.at[0], rx.at[2, zrel, i])
                landed(part.at[1], rx.at[3, zrel, i])
            if not zrel:
                if_late(i, lambda: act(remote(part, part, s_z.at[2, i], rz.at[3, i], across, hd)))
            share(act, x_far, zo, i)

        def last(i, n, xo):
            if waiting:
                landed(piece_of(xo, zp, i), rz.at[n, i])
            share(act, xo, zp, i)

        for i in ARRIVAL:
            if_early(i, lambda: from_across(i))
        for i in ARRIVAL:
            from_side(i, 0, z)
        for i in ARRIVAL:
            if_early(i, lambda: from_side(i, 1, zp))
        for i in ARRIVAL:
            from_far(i, 0, z)
            if waiting:
                between(i)
        for i in ARRIVAL:
            if_early(i, lambda: from_far(i, 1, zp))
        for n, xo in enumerate((x, x_left, x_right, x_far)):
            for i in ARRIVAL:
                if_late(i, lambda: last(i, n, xo))

    ones = jnp.ones((KEYS, WIDTH), jnp.bfloat16)

    def slot_of(i):
        return 2 * chip(x, jnp.where(jnp.int32(i) >= 4, 3 - z, z), (y + i % 4) % 4) + hd

    def queries_of(i):
        whole = q_buf[i]
        return jnp.concatenate([whole[:, g * WIDTH:(g + 1) * WIDTH] for g in range(GROUP)], axis=0)

    def score(q, keys):
        return lax.dot_general(q, keys, (((1,), (1,)), ((), ())), preferred_element_type=jnp.float32)

    def own(i):
        landed(q_buf.at[i], rq.at[i])
        slot = slot_of(i)
        begin = span_ref[slot] * SPAN
        row = lax.broadcasted_iota(jnp.int32, (SPAN, WIDTH), 0)
        low = jnp.zeros((SPAN, WIDTH), jnp.int32)
        for d in range(1, DOCS):
            start = index[1, d]
            low = jnp.maximum(low, jnp.where(start <= begin + row, start, 0))
        low = low - begin
        penalty[i] = jnp.where(low < 0, 0.0, -NEG)
        key = lax.broadcasted_iota(jnp.int32, (SPAN, WIDTH), 1)
        bias = jnp.where((key >= low) & (key <= row), 0.0, NEG)[:, :SPAN]
        s = score(queries_of(i), kv[slot, 0]) + jnp.concatenate([bias] * GROUP, axis=0)
        top = jnp.max(s, axis=1, keepdims=True)
        weights = jnp.exp2(s * FACTOR - top * FACTOR).astype(jnp.bfloat16)
        own_top[i] = jnp.broadcast_to(top, (ROWS, WIDTH))
        values = jnp.concatenate([kv[slot, 1], ones[:SPAN]], axis=1)
        own_acc[i] = jnp.dot(weights, values, preferred_element_type=jnp.float32)

    table_copy.start()
    table_copy.wait()
    place = lax.broadcasted_iota(jnp.int32, (1, BACK * SPAN), 1)
    place_of[...] = place - 2 * SPAN * (place // SPAN)
    relay(go, own)

    def shared(s, carry):
        landed(kv.at[2 * s + other], rd.at[s])
        return carry

    lax.fori_loop(0, 64, shared, 0)

    def give_back(act, i):
        to = chip(x, jnp.where(i >= 4, 3 - z, z), (y + i % 4) % 4)
        act(remote(o_buf.at[i], attn.at[my_rows, my_queries], so.at[i], ro.at[hd * 4 + y], to, z // 2))

    def slot_at(place):
        return jnp.clip(index[0, jnp.clip(place, 0, 127)], 0, 127)

    def block_of(c, t, which):
        parts = []
        for tile in range(256 * t // SPAN, (256 * t + 255) // SPAN + 1):
            first, last = max(256 * t - SPAN * tile, 0), min(256 * t + 256 - SPAN * tile, SPAN)
            parts.append(kv[slot_at(c - 1 - tile), which, first:last])
        return jnp.concatenate(parts, axis=0)

    def turn(n):
        i = jnp.int32(0)
        for k, piece in enumerate(RETURN):
            i = jnp.where(n == k, piece, i)
        return i

    def stage(ahead, now):
        if ahead is not None:
            n, s_a, shift_a, fade_a = ahead
            i = turn(n)
            c = span_ref[slot_of(i)]
            begin = c * SPAN
            low = jnp.int32(0)
            for d in range(1, DOCS):
                start = index[1, d]
                low = jnp.maximum(low, jnp.where(start <= begin, start, 0))
            q = queries_of(i)
            reach = low - (begin - SPAN)
            done = 0
        if now is not None:
            nb, s_b, shift_b, fade_b = now
            ib = turn(nb)
            cb = span_ref[slot_of(ib)]
            acc = None

        def raise_peak(t):
            top = s_a[:, t * KEYS:t * KEYS + WIDTH]
            for l in range(1, KEYS // WIDTH):
                top = jnp.maximum(top, s_a[:, t * KEYS + l * WIDTH:t * KEYS + (l + 1) * WIDTH])
            peak[...] = top if t == 0 else jnp.maximum(peak[...], top)

        for t in range(BLOCKS):
            cut = slice(t * 256, (t + 1) * 256)
            if ahead is not None:
                bias = jnp.where(place_of[:, cut] >= reach, 0.0, NEG)
                s_a[:, cut] = score(q, block_of(c, t, 0)) + bias
                if t >= 4 and (t - 4) % 3 == 0:
                    raise_peak((t - 4) // 3)
            if now is not None:
                shift = shift_b[...]
                shift = jnp.concatenate([shift, shift], axis=1)
                weights = jnp.exp2(s_b[:, cut] * FACTOR - shift).astype(jnp.bfloat16)
                values = jnp.concatenate([block_of(cb, t, 1), ones[:256]], axis=1)
                cuts = (slice(0, ROWS),) if ahead is not None else (slice(0, ROWS // 2), slice(ROWS // 2, ROWS))
                parts = [jnp.dot(weights[r], values, preferred_element_type=jnp.float32) for r in cuts]
                acc = parts if acc is None else [a + b for a, b in zip(acc, parts)]
        if ahead is not None:
            raise_peak(BLOCKS // 3 - 1)
            fence = jnp.concatenate([penalty[i]] * GROUP, axis=0)
            mine = own_top[i]
            top = jnp.maximum(jnp.max(peak[...], axis=1, keepdims=True) - fence, mine)
            fade_a[...] = jnp.exp2((mine - top) * FACTOR)
            shift_a[...] = top * FACTOR + fence
        if now is not None:
            fade = fade_b[...]
            acc = jnp.concatenate(acc, axis=0) + own_acc[ib] * jnp.concatenate([fade, fade], axis=1)
            result = (acc[:, :WIDTH] / acc[:, WIDTH:]).astype(jnp.bfloat16)
            for g in range(GROUP):
                o_buf[ib, :, g * WIDTH:(g + 1) * WIDTH] = result[g * SPAN:(g + 1) * SPAN]

    even = (scores0, shift0, fade0)
    odd = (scores1, shift1, fade1)
    stage((jnp.int32(0),) + even, None)

    def pair(k, carry):
        stage((2 * k + 1,) + odd, (2 * k,) + even)
        give_back(go, turn(2 * k))
        stage((2 * k + 2,) + even, (2 * k + 1,) + odd)
        give_back(go, turn(2 * k + 1))
        return carry

    lax.fori_loop(0, PIECES // 2 - 1, pair, 0)
    stage((jnp.int32(PIECES - 1),) + odd, (jnp.int32(PIECES - 2),) + even)
    give_back(go, jnp.int32(RETURN[PIECES - 2]))
    stage(None, (jnp.int32(PIECES - 1),) + odd)

    @pl.when(home)
    def _():
        attn[my_rows, my_queries] = o_buf[0]

    @pl.when(jnp.logical_not(home))
    def _():
        give_back(go, jnp.int32(0))

    for k in range(2):
        for j in range(4):
            @pl.when(jnp.logical_not(home & (hd == k) & (y == j)))
            def _():
                landed(attn.at[pl.ds(k * SPAN, SPAN), pl.ds(j * GROUP * WIDTH, GROUP * WIDTH)], ro.at[k * 4 + j])

    w_load.wait()
    count, width = outgoing.shape[0], outgoing.shape[2]

    def hand_over(n):
        return remote(outgoing.at[n], incoming.at[n], xs.at[n], xr.at[n], me, other)

    @pl.loop(0, count)
    def _(n):
        columns = pl.ds(pl.multiple_of(n * width, width), width)
        product = jnp.dot(attn[...], w_vmem[:, columns], preferred_element_type=jnp.float32)
        upper, lower = product[:SPAN], product[SPAN:]
        first = hd == 0
        outgoing[n] = jnp.where(first, lower, upper).astype(jnp.bfloat16)
        kept[n] = jnp.where(first, upper, lower)
        hand_over(n).start()

    def put(n):
        return pltpu.make_async_copy(result_of.at[n], out_ref.at[:, pl.ds(n * width, width)], out_sem.at[n])

    for n in range(count):
        hand_over(n).wait_recv()
        result_of[n] = (kept[n] + incoming[n].astype(jnp.float32)).astype(jnp.bfloat16)
        if n:
            put(n - 1).start()

    put(count - 1).start()
    scatter(sent, "kv")
    scatter(sent, "q")
    relay(sent)
    for i in range(PIECES):
        if i:
            give_back(sent, jnp.int32(i))
        else:
            pl.when(jnp.logical_not(home))(lambda: give_back(sent, jnp.int32(0)))
    for n in range(count):
        hand_over(n).wait_send()
        put(n).wait()


def local(queries, keys, values, span_table, doc_ids, out_weight):
    model = out_weight.shape[1]
    count = 8
    vmem, hbm = pltpu.VMEM, pl.ANY
    spec = lambda space: pl.BlockSpec(memory_space=space)
    dma = pltpu.SemaphoreType.DMA
    f32, bf16, i32 = jnp.float32, jnp.bfloat16, jnp.int32
    return pl.pallas_call(
        kernel,
        out_shape=jax.ShapeDtypeStruct((SPAN, model), bf16),
        in_specs=[spec(hbm)] * 7,
        out_specs=spec(hbm),
        scratch_shapes=[
            vmem(queries.shape, bf16),
            vmem(keys.shape, bf16),
            vmem(values.shape, bf16),
            vmem((128, 2, SPAN, WIDTH), bf16),
            vmem((PIECES, SPAN, GROUP * WIDTH), bf16),
            vmem((PIECES, SPAN, GROUP * WIDTH), bf16),
            vmem(queries.shape, bf16),
            vmem(out_weight.shape, bf16),
            vmem((ROWS, BACK * SPAN), f32),
            vmem((ROWS, BACK * SPAN), f32),
            vmem((ROWS, WIDTH), f32),
            vmem((ROWS, WIDTH), f32),
            vmem((ROWS, WIDTH), f32),
            vmem((ROWS, WIDTH), f32),
            vmem((ROWS, WIDTH), f32),
            vmem((1, BACK * SPAN), i32),
            vmem((PIECES, ROWS, 2 * WIDTH), f32),
            vmem((PIECES, ROWS, WIDTH), f32),
            vmem((PIECES, SPAN, WIDTH), f32),
            vmem((8, 128), i32),
            vmem((count, SPAN, model // count), bf16),
            vmem((count, SPAN, model // count), bf16),
            vmem((count, SPAN, model // count), f32),
            vmem((count, SPAN, model // count), bf16),
            vmem((1, 128), i32),
            vmem((doc_ids.shape[0] // 128, 128), i32),
            pltpu.SMEM((128,), i32),
            pltpu.SMEM((8, 128), i32),
            dma((3,)), dma((3,)), dma, dma, dma((count,)),
            dma((4, 2, 2)), dma((4, 2)), dma((PIECES, 2)), dma((PIECES,)),
            dma((PIECES, 3)), dma((PIECES, 2)), dma((2, 2, PIECES)), dma((3, PIECES)),
            dma((4, 2, PIECES)), dma((4, PIECES)), dma((64,)), dma((64,)),
            dma((PIECES,)), dma((PIECES,)), dma((count,)), dma((count,)),
        ],
        compiler_params=pltpu.CompilerParams(
            collective_id=0, has_side_effects=True, vmem_limit_bytes=60 * 2 ** 20,
        ),
    )(span_table, span_table.reshape(1, 128), doc_ids.reshape(-1, 128), queries, keys, values, out_weight)


def solution(mesh):
    return jax.shard_map(
        local,
        mesh=mesh,
        in_specs=(P("cp", "hd"), P("cp", "hd"), P("cp", "hd"), P(), P(), P("hd", None)),
        out_specs=P(("cp", "hd"), None),
        check_vma=False,
    )
```

```python
import functools
import math

import jax
import jax.numpy as jnp
from jax import lax
from jax.experimental import pallas as pl
from jax.experimental.pallas import tpu as pltpu
from jax.sharding import PartitionSpec as P

WIDTH = 128
SPAN = 96
GROUP = 4
ROWS = GROUP * SPAN
PIECES = 8
DOCS = 8
BACK = 32
STEP = 8
KEYS = STEP * SPAN
BLOCKS = BACK * SPAN // 256
NEG = -1e30
MESH = pl.DeviceIdType.MESH
FACTOR = WIDTH ** -0.5 * math.log2(math.e)
ARRIVAL = (0, 1, 3, 4, 2, 5, 7, 6)
EARLY = (2, 5, 7, 6)
LATE = (0, 1, 3)
SPLIT = 4
RETURN = (6, 5, 2, 7, 1, 4, 3, 0)


def kernel(
    span_hbm, span_row_hbm, doc_hbm, q_hbm, k_hbm, v_hbm, w_hbm, out_ref,
    q_in, k_in, v_in, kv, q_buf, o_buf, attn, w_vmem, scores0, scores1, shift0, shift1, fade0, fade1, peak, place_of, own_acc, own_top, penalty, table,
    outgoing, incoming, kept, result_of, span_row_ref, doc_ref, span_ref, index,
    load_sem, small_sem, w_sem, table_sem, out_sem,
    su, sq, ru, rq, s_own, s_far, s_half, s_z, rx, rz, sd, rd, so, ro, xs, xr,
):
    me = lax.axis_index("cp")
    hd = lax.axis_index("hd")
    other = 1 - hd
    x, z, y = me // 16, (me // 4) % 4, me % 4
    home = (z // 2) == hd
    zp = z + 1 - 2 * (z % 2)

    def chip(xx, zz, yy):
        return xx * 16 + zz * 4 + yy

    right, left, across = chip((x + 1) % 4, z, y), chip((x + 3) % 4, z, y), chip(x, zp, y)

    def source(xo, zo, i):
        return chip(xo, 3 - zo if i >= 4 else zo, (y + i % 4) % 4)

    def remote(src, dst, send, recv, cp, core):
        return pltpu.make_async_remote_copy(
            src_ref=src, dst_ref=dst, send_sem=send, recv_sem=recv,
            device_id={"cp": cp, "hd": core}, device_id_type=MESH,
        )

    def landed(dst, sem):
        remote(dst, dst, sd.at[0], sem, me, other).wait_recv()

    def go(copy):
        copy.start()

    def sent(copy):
        copy.wait_send()

    my_rows = pl.ds(pl.multiple_of(hd * SPAN, SPAN), SPAN)
    my_head = pl.ds(pl.multiple_of(y * WIDTH, WIDTH), WIDTH)
    my_queries = pl.ds(pl.multiple_of(y * GROUP * WIDTH, GROUP * WIDTH), GROUP * WIDTH)

    loads = [
        pltpu.make_async_copy(k_hbm, k_in, load_sem.at[0]),
        pltpu.make_async_copy(v_hbm, v_in, load_sem.at[1]),
        pltpu.make_async_copy(q_hbm, q_in, load_sem.at[2]),
    ]
    locals_ = [
        pltpu.make_async_copy(k_hbm.at[my_rows, my_head], kv.at[2 * me + hd, 0], ru.at[0, 0]),
        pltpu.make_async_copy(v_hbm.at[my_rows, my_head], kv.at[2 * me + hd, 1], ru.at[0, 1]),
        pltpu.make_async_copy(q_hbm.at[my_rows, my_queries], q_buf.at[0], rq.at[0]),
    ]
    w_load = pltpu.make_async_copy(w_hbm, w_vmem, w_sem)
    small = [
        pltpu.make_async_copy(span_row_hbm, span_row_ref, small_sem.at[0]),
        pltpu.make_async_copy(doc_hbm, doc_ref, small_sem.at[1]),
        pltpu.make_async_copy(span_hbm, span_ref, small_sem.at[2]),
    ]
    for load in loads + small:
        load.start()

    @pl.when(home)
    def _():
        for copy in locals_:
            copy.start()

    barrier = pltpu.get_barrier_semaphore()

    def greet(cp, core):
        pl.semaphore_signal(barrier, inc=1, device_id={"cp": cp, "hd": core}, device_id_type=MESH)

    for i in range(PIECES):
        for core in (hd, other):
            if i or core is other:
                greet(source(x, z, i), core)
    for target in (right, left, across):
        greet(target, hd)

    for load in small:
        load.wait()
    spans = jnp.broadcast_to(span_row_ref[...].astype(jnp.float32), (128, 128)).T
    held_by = lax.broadcasted_iota(jnp.int32, (128, 128), 0).astype(jnp.float32)
    wanted = lax.broadcasted_iota(jnp.int32, (128, 128), 1).astype(jnp.float32)
    table[0:1, :] = jnp.max(jnp.where(spans == wanted, held_by, 0.0), axis=0, keepdims=True).astype(jnp.int32)
    docs = doc_ref[...]
    lane = lax.broadcasted_iota(jnp.int32, (1, 128), 1)
    starts = jnp.zeros((1, 128), jnp.float32)
    for d in range(1, DOCS):
        first = jnp.sum(jnp.where(docs < d, 1.0, 0.0), keepdims=True)
        starts = jnp.where(lane == d, first, starts)
    table[1:2, :] = starts.astype(jnp.int32)

    pl.semaphore_wait(barrier, 2 * PIECES + 2)

    tz = jnp.where(home, z, 3 - z)

    def scatter(act, what):
        for dj in (0, 1, 3, 2):
            j = (y + dj) % 4
            to = chip(x, tz, j)
            piece = jnp.where(home, 0, 4) + (4 - dj) % 4
            for rel, core in enumerate((hd, other)):
                rows = pl.ds(pl.multiple_of(core * SPAN, SPAN), SPAN)

                def one():
                    if what == "kv":
                        columns = pl.ds(pl.multiple_of(j * WIDTH, WIDTH), WIDTH)
                        for v, staged in enumerate((k_in, v_in)):
                            act(remote(staged.at[rows, columns], kv.at[2 * me + core, v],
                                       su.at[dj, rel, v], ru.at[piece, v], to, core))
                    else:
                        columns = pl.ds(pl.multiple_of(j * GROUP * WIDTH, GROUP * WIDTH), GROUP * WIDTH)
                        act(remote(q_in.at[rows, columns], q_buf.at[piece],
                                   sq.at[dj, rel], rq.at[piece], to, core))

                if dj == 0 and rel == 0:
                    pl.when(jnp.logical_not(home))(one)
                else:
                    one()

    loads[0].wait()
    loads[1].wait()
    scatter(go, "kv")
    loads[2].wait()
    scatter(go, "q")
    w_load.start()
    table_copy = pltpu.make_async_copy(table, index, table_sem)

    def piece_of(xo, zo, i):
        return kv.at[2 * source(xo, zo, i) + hd]

    def share(act, xo, zo, i):
        s = source(xo, zo, i)
        part = kv.at[2 * s + hd]
        act(remote(part, part, sd.at[s], rd, me, other))

    x_left, x_right, x_far = (x + 3) % 4, (x + 1) % 4, (x + 2) % 4

    def if_early(i, fn):
        if i == SPLIT:
            pl.when(hd == 0)(fn)
        elif i in EARLY:
            fn()

    def if_late(i, fn):
        if i == SPLIT:
            pl.when(hd == 1)(fn)
        elif i in LATE:
            fn()

    def relay(act, between=None):
        waiting = act is go
        for i in ARRIVAL:
            part = piece_of(x, z, i)
            if waiting:
                landed(part.at[0], ru.at[i, 0])
                landed(part.at[1], ru.at[i, 1])
            act(remote(part, part, s_own.at[i, 0], rx.at[0, 0, i], right, hd))
            act(remote(part, part, s_own.at[i, 1], rx.at[1, 0, i], left, hd))
            act(remote(part, part, s_own.at[i, 2], rz.at[0, i], across, hd))
            share(act, x, z, i)

        def from_across(i):
            part = piece_of(x, zp, i)
            if waiting:
                landed(part, rz.at[0, i])
            act(remote(part, part, s_far.at[i, 0], rx.at[0, 1, i], right, hd))
            act(remote(part, part, s_far.at[i, 1], rx.at[1, 1, i], left, hd))
            share(act, x, zp, i)

        def from_side(i, zrel, zo):
            for side, xo, onward, half in ((0, x_left, right, 0), (1, x_right, left, 1)):
                part = piece_of(xo, zo, i)
                if waiting:
                    landed(part, rx.at[side, zrel, i])
                act(remote(part.at[half], part.at[half], s_half.at[side, zrel, i],
                           rx.at[2 + side, zrel, i], onward, hd))
                if not zrel:
                    if_late(i, lambda: act(remote(part, part, s_z.at[side, i], rz.at[1 + side, i], across, hd)))
                share(act, xo, zo, i)

        def from_far(i, zrel, zo):
            part = piece_of(x_far, zo, i)
            if waiting:
                landed(part.at[0], rx.at[2, zrel, i])
                landed(part.at[1], rx.at[3, zrel, i])
            if not zrel:
                if_late(i, lambda: act(remote(part, part, s_z.at[2, i], rz.at[3, i], across, hd)))
            share(act, x_far, zo, i)

        def last(i, n, xo):
            if waiting:
                landed(piece_of(xo, zp, i), rz.at[n, i])
            share(act, xo, zp, i)

        def extra(k):
            if waiting:
                between(ARRIVAL[k])

        near = LATE + (SPLIT,)
        for i in near:
            if_late(i, lambda: from_side(i, 0, z))
        for i in (SPLIT,) + EARLY:
            if_early(i, lambda: from_across(i))
        for i in near:
            if_late(i, lambda: from_far(i, 0, z))
        for i in (SPLIT,) + EARLY:
            if_early(i, lambda: from_side(i, 0, z))
        for k, i in enumerate((SPLIT,) + EARLY):
            if_early(i, lambda: from_side(i, 1, zp))
            if k:
                extra(k - 1)
        for k, i in enumerate((SPLIT,) + EARLY):
            if_early(i, lambda: from_far(i, 0, z))
            if k:
                extra(k + 3)
        for n, xo in enumerate((x, x_left, x_right, x_far)):
            for i in near:
                if_late(i, lambda: last(i, n, xo))
        for i in (SPLIT,) + EARLY:
            if_early(i, lambda: from_far(i, 1, zp))

    ones = jnp.ones((KEYS, WIDTH), jnp.bfloat16)

    def slot_of(i):
        return 2 * chip(x, jnp.where(jnp.int32(i) >= 4, 3 - z, z), (y + i % 4) % 4) + hd

    def queries_of(i):
        whole = q_buf[i]
        return jnp.concatenate([whole[:, g * WIDTH:(g + 1) * WIDTH] for g in range(GROUP)], axis=0)

    def score(q, keys):
        return lax.dot_general(q, keys, (((1,), (1,)), ((), ())), preferred_element_type=jnp.float32)

    def own(i):
        landed(q_buf.at[i], rq.at[i])
        slot = slot_of(i)
        begin = span_ref[slot] * SPAN
        row = lax.broadcasted_iota(jnp.int32, (SPAN, WIDTH), 0)
        low = jnp.zeros((SPAN, WIDTH), jnp.int32)
        for d in range(1, DOCS):
            start = index[1, d]
            low = jnp.maximum(low, jnp.where(start <= begin + row, start, 0))
        low = low - begin
        penalty[i] = jnp.where(low < 0, 0.0, -NEG)
        key = lax.broadcasted_iota(jnp.int32, (SPAN, WIDTH), 1)
        bias = jnp.where((key >= low) & (key <= row), 0.0, NEG)[:, :SPAN]
        s = score(queries_of(i), kv[slot, 0]) + jnp.concatenate([bias] * GROUP, axis=0)
        top = jnp.max(s, axis=1, keepdims=True)
        weights = jnp.exp2(s * FACTOR - top * FACTOR).astype(jnp.bfloat16)
        own_top[i] = jnp.broadcast_to(top, (ROWS, WIDTH))
        values = jnp.concatenate([kv[slot, 1], ones[:SPAN]], axis=1)
        own_acc[i] = jnp.dot(weights, values, preferred_element_type=jnp.float32)

    table_copy.start()
    table_copy.wait()
    place = lax.broadcasted_iota(jnp.int32, (1, BACK * SPAN), 1)
    place_of[...] = place - 2 * SPAN * (place // SPAN)
    relay(go, own)

    landed(kv.at[pl.ds(0, 64)], rd)

    def give_back(act, i):
        to = chip(x, jnp.where(i >= 4, 3 - z, z), (y + i % 4) % 4)
        act(remote(o_buf.at[i], attn.at[my_rows, my_queries], so.at[i], ro.at[hd * 4 + y], to, z // 2))

    def slot_at(place):
        return jnp.clip(index[0, jnp.clip(place, 0, 127)], 0, 127)

    def block_of(c, t, which):
        parts = []
        for tile in range(256 * t // SPAN, (256 * t + 255) // SPAN + 1):
            first, last = max(256 * t - SPAN * tile, 0), min(256 * t + 256 - SPAN * tile, SPAN)
            parts.append(kv[slot_at(c - 1 - tile), which, first:last])
        return jnp.concatenate(parts, axis=0)

    def turn(n):
        i = jnp.int32(0)
        for k, piece in enumerate(RETURN):
            i = jnp.where(n == k, piece, i)
        return i

    def stage(ahead, now):
        if ahead is not None:
            n, s_a, shift_a, fade_a = ahead
            i = turn(n)
            c = span_ref[slot_of(i)]
            begin = c * SPAN
            low = jnp.int32(0)
            for d in range(1, DOCS):
                start = index[1, d]
                low = jnp.maximum(low, jnp.where(start <= begin, start, 0))
            q = queries_of(i)
            reach = low - (begin - SPAN)
            done = 0
        if now is not None:
            nb, s_b, shift_b, fade_b = now
            ib = turn(nb)
            cb = span_ref[slot_of(ib)]
            acc = {}

        def raise_peak(t):
            top = s_a[:, t * KEYS:t * KEYS + WIDTH]
            for l in range(1, KEYS // WIDTH):
                top = jnp.maximum(top, s_a[:, t * KEYS + l * WIDTH:t * KEYS + (l + 1) * WIDTH])
            peak[...] = top if t == 0 else jnp.maximum(peak[...], top)

        for t in range(BLOCKS):
            cut = slice(t * 256, (t + 1) * 256)
            if ahead is not None:
                bias = jnp.where(place_of[:, cut] >= reach, 0.0, NEG)
                s_a[:, cut] = score(q, block_of(c, t, 0)) + bias
                if t >= 4 and (t - 4) % 3 == 0:
                    raise_peak((t - 4) // 3)
            if now is not None:
                shift = shift_b[...]
                shift = jnp.concatenate([shift, shift], axis=1)
                weights = jnp.exp2(s_b[:, cut] * FACTOR - shift).astype(jnp.bfloat16)
                values = jnp.concatenate([block_of(cb, t, 1), ones[:256]], axis=1)
                part = jnp.dot(weights, values, preferred_element_type=jnp.float32)
                chain = 0 if ahead is not None else t % 2
                acc[chain] = acc[chain] + part if chain in acc else part
        if ahead is not None:
            raise_peak(BLOCKS // 3 - 1)
            fence = jnp.concatenate([penalty[i]] * GROUP, axis=0)
            mine = own_top[i]
            top = jnp.maximum(jnp.max(peak[...], axis=1, keepdims=True) - fence, mine)
            fade_a[...] = jnp.exp2((mine - top) * FACTOR)
            shift_a[...] = top * FACTOR + fence
        if now is not None:
            fade = fade_b[...]
            if 1 in acc:
                scores0[:, :2 * WIDTH] = acc[0]
                acc = {0: acc[1] + scores0[:, :2 * WIDTH]}
            acc = acc[0] + own_acc[ib] * jnp.concatenate([fade, fade], axis=1)
            result = (acc[:, :WIDTH] / acc[:, WIDTH:]).astype(jnp.bfloat16)
            for g in range(GROUP):
                o_buf[ib, :, g * WIDTH:(g + 1) * WIDTH] = result[g * SPAN:(g + 1) * SPAN]

    even = (scores0, shift0, fade0)
    odd = (scores1, shift1, fade1)
    stage((jnp.int32(0),) + even, None)

    def pair(k, carry):
        stage((2 * k + 1,) + odd, (2 * k,) + even)
        give_back(go, turn(2 * k))
        stage((2 * k + 2,) + even, (2 * k + 1,) + odd)
        give_back(go, turn(2 * k + 1))
        return carry

    lax.fori_loop(0, PIECES // 2 - 1, pair, 0)
    stage((jnp.int32(PIECES - 1),) + odd, (jnp.int32(PIECES - 2),) + even)
    give_back(go, turn(jnp.int32(PIECES - 2)))
    stage(None, (jnp.int32(PIECES - 1),) + odd)

    @pl.when(home)
    def _():
        attn[my_rows, my_queries] = o_buf[0]

    @pl.when(jnp.logical_not(home))
    def _():
        give_back(go, jnp.int32(0))

    scatter(sent, "kv")
    scatter(sent, "q")
    relay(sent)

    for k in range(2):
        for j in range(4):
            @pl.when(jnp.logical_not(home & (hd == k) & (y == j)))
            def _():
                landed(attn.at[pl.ds(k * SPAN, SPAN), pl.ds(j * GROUP * WIDTH, GROUP * WIDTH)], ro.at[k * 4 + j])

    w_load.wait()
    count, width = outgoing.shape[0], outgoing.shape[2]

    def hand_over(n):
        return remote(outgoing.at[n], incoming.at[n], xs.at[n], xr.at[n], me, other)

    @pl.loop(0, count)
    def _(n):
        columns = pl.ds(pl.multiple_of(n * width, width), width)
        product = jnp.dot(attn[...], w_vmem[:, columns], preferred_element_type=jnp.float32)
        upper, lower = product[:SPAN], product[SPAN:]
        first = hd == 0
        outgoing[n] = jnp.where(first, lower, upper).astype(jnp.bfloat16)
        kept[n] = jnp.where(first, upper, lower)
        hand_over(n).start()

    for i in range(PIECES):
        if i:
            give_back(sent, jnp.int32(i))
        else:
            pl.when(jnp.logical_not(home))(lambda: give_back(sent, jnp.int32(0)))

    def put(n):
        return pltpu.make_async_copy(result_of.at[n], out_ref.at[:, pl.ds(n * width, width)], out_sem.at[n])

    for n in range(count):
        hand_over(n).wait_recv()
        result_of[n] = (kept[n] + incoming[n].astype(jnp.float32)).astype(jnp.bfloat16)
        if n:
            put(n - 1).start()

    put(count - 1).start()
    for n in range(count):
        hand_over(n).wait_send()
        put(n).wait()


def local(queries, keys, values, span_table, doc_ids, out_weight):
    model = out_weight.shape[1]
    count = 8
    vmem, hbm = pltpu.VMEM, pl.ANY
    spec = lambda space: pl.BlockSpec(memory_space=space)
    dma = pltpu.SemaphoreType.DMA
    f32, bf16, i32 = jnp.float32, jnp.bfloat16, jnp.int32
    return pl.pallas_call(
        kernel,
        out_shape=jax.ShapeDtypeStruct((SPAN, model), bf16),
        in_specs=[spec(hbm)] * 7,
        out_specs=spec(hbm),
        scratch_shapes=[
            vmem(queries.shape, bf16),
            vmem(keys.shape, bf16),
            vmem(values.shape, bf16),
            vmem((128, 2, SPAN, WIDTH), bf16),
            vmem((PIECES, SPAN, GROUP * WIDTH), bf16),
            vmem((PIECES, SPAN, GROUP * WIDTH), bf16),
            vmem(queries.shape, bf16),
            vmem(out_weight.shape, bf16),
            vmem((ROWS, BACK * SPAN), f32),
            vmem((ROWS, BACK * SPAN), f32),
            vmem((ROWS, WIDTH), f32),
            vmem((ROWS, WIDTH), f32),
            vmem((ROWS, WIDTH), f32),
            vmem((ROWS, WIDTH), f32),
            vmem((ROWS, WIDTH), f32),
            vmem((1, BACK * SPAN), i32),
            vmem((PIECES, ROWS, 2 * WIDTH), f32),
            vmem((PIECES, ROWS, WIDTH), f32),
            vmem((PIECES, SPAN, WIDTH), f32),
            vmem((8, 128), i32),
            vmem((count, SPAN, model // count), bf16),
            vmem((count, SPAN, model // count), bf16),
            vmem((count, SPAN, model // count), f32),
            vmem((count, SPAN, model // count), bf16),
            vmem((1, 128), i32),
            vmem((doc_ids.shape[0] // 128, 128), i32),
            pltpu.SMEM((128,), i32),
            pltpu.SMEM((8, 128), i32),
            dma((3,)), dma((3,)), dma, dma, dma((count,)),
            dma((4, 2, 2)), dma((4, 2)), dma((PIECES, 2)), dma((PIECES,)),
            dma((PIECES, 3)), dma((PIECES, 2)), dma((2, 2, PIECES)), dma((3, PIECES)),
            dma((4, 2, PIECES)), dma((4, PIECES)), dma((64,)), dma,
            dma((PIECES,)), dma((PIECES,)), dma((count,)), dma((count,)),
        ],
        compiler_params=pltpu.CompilerParams(
            collective_id=0, has_side_effects=True, vmem_limit_bytes=60 * 2 ** 20,
        ),
    )(span_table, span_table.reshape(1, 128), doc_ids.reshape(-1, 128), queries, keys, values, out_weight)


def solution(mesh):
    return jax.shard_map(
        local,
        mesh=mesh,
        in_specs=(P("cp", "hd"), P("cp", "hd"), P("cp", "hd"), P(), P(), P("hd", None)),
        out_specs=P(("cp", "hd"), None),
        check_vma=False,
    )
```

```python
import functools
import math

import jax
import jax.numpy as jnp
from jax import lax
from jax.experimental import pallas as pl
from jax.experimental.pallas import tpu as pltpu
from jax.sharding import PartitionSpec as P

WIDTH = 128
SPAN = 96
GROUP = 4
ROWS = GROUP * SPAN
PIECES = 8
DOCS = 8
BACK = 32
STEP = 8
KEYS = STEP * SPAN
BLOCKS = BACK * SPAN // 256
NEG = -1e30
MESH = pl.DeviceIdType.MESH
FACTOR = WIDTH ** -0.5 * math.log2(math.e)
ARRIVAL = (0, 1, 3, 4, 2, 5, 7, 6)
EARLY = (2, 5, 7, 6)
LATE = (0, 1, 3, 4)
RETURN = (6, 5, 2, 7, 1, 4, 3, 0)


def kernel(
    span_hbm, span_row_hbm, doc_hbm, q_hbm, k_hbm, v_hbm, w_hbm, out_ref,
    q_in, k_in, v_in, kv, q_buf, o_buf, attn, w_vmem, scores0, scores1, shift0, shift1, fade0, fade1, peak, place_of, own_acc, own_top, penalty, table,
    outgoing, incoming, kept, result_of, span_row_ref, doc_ref, span_ref, index,
    load_sem, small_sem, w_sem, table_sem, out_sem,
    su, sq, ru, rq, s_own, s_far, s_half, s_z, rx, rz, sd, rd, so, ro, xs, xr,
):
    me = lax.axis_index("cp")
    hd = lax.axis_index("hd")
    other = 1 - hd
    x, z, y = me // 16, (me // 4) % 4, me % 4
    home = (z // 2) == hd
    zp = z + 1 - 2 * (z % 2)

    def chip(xx, zz, yy):
        return xx * 16 + zz * 4 + yy

    right, left, across = chip((x + 1) % 4, z, y), chip((x + 3) % 4, z, y), chip(x, zp, y)

    def source(xo, zo, i):
        return chip(xo, 3 - zo if i >= 4 else zo, (y + i % 4) % 4)

    def remote(src, dst, send, recv, cp, core):
        return pltpu.make_async_remote_copy(
            src_ref=src, dst_ref=dst, send_sem=send, recv_sem=recv,
            device_id={"cp": cp, "hd": core}, device_id_type=MESH,
        )

    def landed(dst, sem):
        remote(dst, dst, sd.at[0], sem, me, other).wait_recv()

    def go(copy):
        copy.start()

    def sent(copy):
        copy.wait_send()

    my_rows = pl.ds(pl.multiple_of(hd * SPAN, SPAN), SPAN)
    my_head = pl.ds(pl.multiple_of(y * WIDTH, WIDTH), WIDTH)
    my_queries = pl.ds(pl.multiple_of(y * GROUP * WIDTH, GROUP * WIDTH), GROUP * WIDTH)

    loads = [
        pltpu.make_async_copy(k_hbm, k_in, load_sem.at[0]),
        pltpu.make_async_copy(v_hbm, v_in, load_sem.at[1]),
        pltpu.make_async_copy(q_hbm, q_in, load_sem.at[2]),
    ]
    locals_ = [
        pltpu.make_async_copy(k_hbm.at[my_rows, my_head], kv.at[2 * me + hd, 0], ru.at[0, 0]),
        pltpu.make_async_copy(v_hbm.at[my_rows, my_head], kv.at[2 * me + hd, 1], ru.at[0, 1]),
        pltpu.make_async_copy(q_hbm.at[my_rows, my_queries], q_buf.at[0], rq.at[0]),
    ]
    w_load = pltpu.make_async_copy(w_hbm, w_vmem, w_sem)
    small = [
        pltpu.make_async_copy(span_row_hbm, span_row_ref, small_sem.at[0]),
        pltpu.make_async_copy(doc_hbm, doc_ref, small_sem.at[1]),
        pltpu.make_async_copy(span_hbm, span_ref, small_sem.at[2]),
    ]
    for load in loads + small:
        load.start()

    @pl.when(home)
    def _():
        for copy in locals_:
            copy.start()

    barrier = pltpu.get_barrier_semaphore()

    def greet(cp, core):
        pl.semaphore_signal(barrier, inc=1, device_id={"cp": cp, "hd": core}, device_id_type=MESH)

    for i in range(PIECES):
        for core in (hd, other):
            if i or core is other:
                greet(source(x, z, i), core)
    for target in (right, left, across):
        greet(target, hd)

    for load in small:
        load.wait()
    spans = jnp.broadcast_to(span_row_ref[...].astype(jnp.float32), (128, 128)).T
    held_by = lax.broadcasted_iota(jnp.int32, (128, 128), 0).astype(jnp.float32)
    wanted = lax.broadcasted_iota(jnp.int32, (128, 128), 1).astype(jnp.float32)
    table[0:1, :] = jnp.max(jnp.where(spans == wanted, held_by, 0.0), axis=0, keepdims=True).astype(jnp.int32)
    docs = doc_ref[...]
    lane = lax.broadcasted_iota(jnp.int32, (1, 128), 1)
    starts = jnp.zeros((1, 128), jnp.float32)
    for d in range(1, DOCS):
        first = jnp.sum(jnp.where(docs < d, 1.0, 0.0), keepdims=True)
        starts = jnp.where(lane == d, first, starts)
    table[1:2, :] = starts.astype(jnp.int32)

    pl.semaphore_wait(barrier, 2 * PIECES + 2)

    tz = jnp.where(home, z, 3 - z)

    def scatter(act, what):
        for dj in (0, 1, 3, 2):
            j = (y + dj) % 4
            to = chip(x, tz, j)
            piece = jnp.where(home, 0, 4) + (4 - dj) % 4
            for rel, core in enumerate((hd, other)):
                rows = pl.ds(pl.multiple_of(core * SPAN, SPAN), SPAN)

                def one():
                    if what == "kv":
                        columns = pl.ds(pl.multiple_of(j * WIDTH, WIDTH), WIDTH)
                        for v, staged in enumerate((k_in, v_in)):
                            act(remote(staged.at[rows, columns], kv.at[2 * me + core, v],
                                       su.at[dj, rel, v], ru.at[piece, v], to, core))
                    else:
                        columns = pl.ds(pl.multiple_of(j * GROUP * WIDTH, GROUP * WIDTH), GROUP * WIDTH)
                        act(remote(q_in.at[rows, columns], q_buf.at[piece],
                                   sq.at[dj, rel], rq.at[piece], to, core))

                if dj == 0 and rel == 0:
                    pl.when(jnp.logical_not(home))(one)
                else:
                    one()

    loads[0].wait()
    loads[1].wait()
    scatter(go, "kv")
    loads[2].wait()
    scatter(go, "q")
    w_load.start()
    table_copy = pltpu.make_async_copy(table, index, table_sem)

    def piece_of(xo, zo, i):
        return kv.at[2 * source(xo, zo, i) + hd]

    def share(act, xo, zo, i):
        s = source(xo, zo, i)
        part = kv.at[2 * s + hd]
        act(remote(part, part, sd.at[s], rd, me, other))

    x_left, x_right, x_far = (x + 3) % 4, (x + 1) % 4, (x + 2) % 4

    def relay(act, between=None):
        waiting = act is go
        for i in ARRIVAL:
            part = piece_of(x, z, i)
            if waiting:
                landed(part.at[0], ru.at[i, 0])
                landed(part.at[1], ru.at[i, 1])
            act(remote(part, part, s_own.at[i, 0], rx.at[0, 0, i], right, hd))
            act(remote(part, part, s_own.at[i, 1], rx.at[1, 0, i], left, hd))
            act(remote(part, part, s_own.at[i, 2], rz.at[0, i], across, hd))
            share(act, x, z, i)

        def from_across(i):
            part = piece_of(x, zp, i)
            if waiting:
                landed(part, rz.at[0, i])
            act(remote(part, part, s_far.at[i, 0], rx.at[0, 1, i], right, hd))
            act(remote(part, part, s_far.at[i, 1], rx.at[1, 1, i], left, hd))
            share(act, x, zp, i)

        def from_side(i, zrel, zo):
            for side, xo, onward, half in ((0, x_left, right, 0), (1, x_right, left, 1)):
                part = piece_of(xo, zo, i)
                if waiting:
                    landed(part, rx.at[side, zrel, i])
                act(remote(part.at[half], part.at[half], s_half.at[side, zrel, i],
                           rx.at[2 + side, zrel, i], onward, hd))
                if not zrel and i in LATE:
                    act(remote(part, part, s_z.at[side, i], rz.at[1 + side, i], across, hd))
                share(act, xo, zo, i)

        def from_far(i, zrel, zo):
            part = piece_of(x_far, zo, i)
            if waiting:
                landed(part.at[0], rx.at[2, zrel, i])
                landed(part.at[1], rx.at[3, zrel, i])
            if not zrel and i in LATE:
                act(remote(part, part, s_z.at[2, i], rz.at[3, i], across, hd))
            share(act, x_far, zo, i)

        def last(i, n, xo):
            if waiting:
                landed(piece_of(xo, zp, i), rz.at[n, i])
            share(act, xo, zp, i)

        def extra(k):
            if waiting:
                between(ARRIVAL[k])

        for i in LATE:
            from_side(i, 0, z)
        for i in EARLY:
            from_across(i)
        for i in LATE:
            from_far(i, 0, z)
        for i in EARLY:
            from_side(i, 0, z)
        for k, i in enumerate(EARLY):
            from_side(i, 1, zp)
            extra(k)
        for k, i in enumerate(EARLY):
            from_far(i, 0, z)
            extra(k + 4)
        for n, xo in enumerate((x, x_left, x_right, x_far)):
            for i in LATE:
                last(i, n, xo)
        for i in EARLY:
            from_far(i, 1, zp)

    ones = jnp.ones((KEYS, WIDTH), jnp.bfloat16)

    def slot_of(i):
        return 2 * chip(x, jnp.where(jnp.int32(i) >= 4, 3 - z, z), (y + i % 4) % 4) + hd

    def queries_of(i):
        whole = q_buf[i]
        return jnp.concatenate([whole[:, g * WIDTH:(g + 1) * WIDTH] for g in range(GROUP)], axis=0)

    def score(q, keys):
        return lax.dot_general(q, keys, (((1,), (1,)), ((), ())), preferred_element_type=jnp.float32)

    def own(i):
        landed(q_buf.at[i], rq.at[i])
        slot = slot_of(i)
        begin = span_ref[slot] * SPAN
        row = lax.broadcasted_iota(jnp.int32, (SPAN, WIDTH), 0)
        low = jnp.zeros((SPAN, WIDTH), jnp.int32)
        for d in range(1, DOCS):
            start = index[1, d]
            low = jnp.maximum(low, jnp.where(start <= begin + row, start, 0))
        low = low - begin
        penalty[i] = jnp.where(low < 0, 0.0, -NEG)
        key = lax.broadcasted_iota(jnp.int32, (SPAN, WIDTH), 1)
        bias = jnp.where((key >= low) & (key <= row), 0.0, NEG)[:, :SPAN]
        s = score(queries_of(i), kv[slot, 0]) + jnp.concatenate([bias] * GROUP, axis=0)
        top = jnp.max(s, axis=1, keepdims=True)
        weights = jnp.exp2(s * FACTOR - top * FACTOR).astype(jnp.bfloat16)
        own_top[i] = jnp.broadcast_to(top, (ROWS, WIDTH))
        values = jnp.concatenate([kv[slot, 1], ones[:SPAN]], axis=1)
        own_acc[i] = jnp.dot(weights, values, preferred_element_type=jnp.float32)

    table_copy.start()
    table_copy.wait()
    place = lax.broadcasted_iota(jnp.int32, (1, BACK * SPAN), 1)
    place_of[...] = place - 2 * SPAN * (place // SPAN)
    relay(go, own)

    landed(kv.at[pl.ds(0, 64)], rd)

    def give_back(act, i):
        to = chip(x, jnp.where(i >= 4, 3 - z, z), (y + i % 4) % 4)
        act(remote(o_buf.at[i], attn.at[my_rows, my_queries], so.at[i], ro.at[hd * 4 + y], to, z // 2))

    def slot_at(place):
        return jnp.clip(index[0, jnp.clip(place, 0, 127)], 0, 127)

    def block_of(c, t, which):
        parts = []
        for tile in range(256 * t // SPAN, (256 * t + 255) // SPAN + 1):
            first, last = max(256 * t - SPAN * tile, 0), min(256 * t + 256 - SPAN * tile, SPAN)
            parts.append(kv[slot_at(c - 1 - tile), which, first:last])
        return jnp.concatenate(parts, axis=0)

    def turn(n):
        i = jnp.int32(0)
        for k, piece in enumerate(RETURN):
            i = jnp.where(n == k, piece, i)
        return i

    def stage(ahead, now, before=None):
        if ahead is not None:
            n, s_a, shift_a, fade_a = ahead
            i = turn(n)
            c = span_ref[slot_of(i)]
            begin = c * SPAN
            low = jnp.int32(0)
            for d in range(1, DOCS):
                start = index[1, d]
                low = jnp.maximum(low, jnp.where(start <= begin, start, 0))
            q = queries_of(i)
            reach = low - (begin - SPAN)
            done = 0
        if now is not None:
            nb, s_b, shift_b, fade_b = now
            ib = turn(nb)
            cb = span_ref[slot_of(ib)]
            acc = {}

        def raise_peak(t):
            top = s_a[:, t * KEYS:t * KEYS + WIDTH]
            for l in range(1, KEYS // WIDTH):
                top = jnp.maximum(top, s_a[:, t * KEYS + l * WIDTH:t * KEYS + (l + 1) * WIDTH])
            peak[...] = top if t == 0 else jnp.maximum(peak[...], top)

        for t in range(BLOCKS):
            cut = slice(t * 256, (t + 1) * 256)
            if ahead is not None:
                bias = jnp.where(place_of[:, cut] >= reach, 0.0, NEG)
                s_a[:, cut] = score(q, block_of(c, t, 0)) + bias
                if t >= 4 and (t - 4) % 3 == 0:
                    raise_peak((t - 4) // 3)
            if now is not None:
                shift = shift_b[...]
                shift = jnp.concatenate([shift, shift], axis=1)
                weights = jnp.exp2(s_b[:, cut] * FACTOR - shift).astype(jnp.bfloat16)
                values = jnp.concatenate([block_of(cb, t, 1), ones[:256]], axis=1)
                part = jnp.dot(weights, values, preferred_element_type=jnp.float32)
                chain = 0 if ahead is not None else t % 2
                acc[chain] = acc[chain] + part if chain in acc else part
        if ahead is not None:
            raise_peak(BLOCKS // 3 - 1)
            fence = jnp.concatenate([penalty[i]] * GROUP, axis=0)
            mine = own_top[i]
            top = jnp.maximum(jnp.max(peak[...], axis=1, keepdims=True) - fence, mine)
            fade_a[...] = jnp.exp2((mine - top) * FACTOR)
            shift_a[...] = top * FACTOR + fence
        if now is not None:
            fade = fade_b[...]
            if 1 in acc:
                scores0[:, :2 * WIDTH] = acc[0]
                acc = {0: acc[1] + scores0[:, :2 * WIDTH]}
            acc = acc[0] + own_acc[ib] * jnp.concatenate([fade, fade], axis=1)
            result = (acc[:, :WIDTH] / acc[:, WIDTH:]).astype(jnp.bfloat16)
            for g in range(GROUP):
                o_buf[ib, :, g * WIDTH:(g + 1) * WIDTH] = result[g * SPAN:(g + 1) * SPAN]

    even = (scores0, shift0, fade0)
    odd = (scores1, shift1, fade1)
    stage((jnp.int32(0),) + even, None)
    stage((jnp.int32(1),) + odd, (jnp.int32(0),) + even)
    give_back(go, turn(jnp.int32(0)))

    def pair(k, carry):
        stage((2 * k + 2,) + even, (2 * k + 1,) + odd)
        give_back(go, turn(2 * k + 1))
        stage((2 * k + 3,) + odd, (2 * k + 2,) + even)
        give_back(go, turn(2 * k + 2))
        return carry

    lax.fori_loop(0, PIECES // 2 - 1, pair, 0)
    stage(None, (jnp.int32(PIECES - 1),) + odd)

    @pl.when(home)
    def _():
        attn[my_rows, my_queries] = o_buf[0]

    @pl.when(jnp.logical_not(home))
    def _():
        give_back(go, jnp.int32(0))

    scatter(sent, "kv")
    scatter(sent, "q")
    relay(sent)

    for k in range(2):
        for j in range(4):
            @pl.when(jnp.logical_not(home & (hd == k) & (y == j)))
            def _():
                landed(attn.at[pl.ds(k * SPAN, SPAN), pl.ds(j * GROUP * WIDTH, GROUP * WIDTH)], ro.at[k * 4 + j])

    w_load.wait()
    count, width = outgoing.shape[0], outgoing.shape[2]

    def hand_over(n):
        return remote(outgoing.at[n], incoming.at[n], xs.at[n], xr.at[n], me, other)

    @pl.loop(0, count)
    def _(n):
        columns = pl.ds(pl.multiple_of(n * width, width), width)
        product = jnp.dot(attn[...], w_vmem[:, columns], preferred_element_type=jnp.float32)
        upper, lower = product[:SPAN], product[SPAN:]
        first = hd == 0
        outgoing[n] = jnp.where(first, lower, upper).astype(jnp.bfloat16)
        kept[n] = jnp.where(first, upper, lower)
        hand_over(n).start()

    for i in range(PIECES):
        if i:
            give_back(sent, jnp.int32(i))
        else:
            pl.when(jnp.logical_not(home))(lambda: give_back(sent, jnp.int32(0)))

    def put(n):
        return pltpu.make_async_copy(result_of.at[n], out_ref.at[:, pl.ds(n * width, width)], out_sem.at[n])

    for n in range(count):
        hand_over(n).wait_recv()
        result_of[n] = (kept[n] + incoming[n].astype(jnp.float32)).astype(jnp.bfloat16)
        if n:
            put(n - 1).start()

    put(count - 1).start()
    for n in range(count):
        hand_over(n).wait_send()
        put(n).wait()


def local(queries, keys, values, span_table, doc_ids, out_weight):
    model = out_weight.shape[1]
    count = 8
    vmem, hbm = pltpu.VMEM, pl.ANY
    spec = lambda space: pl.BlockSpec(memory_space=space)
    dma = pltpu.SemaphoreType.DMA
    f32, bf16, i32 = jnp.float32, jnp.bfloat16, jnp.int32
    return pl.pallas_call(
        kernel,
        out_shape=jax.ShapeDtypeStruct((SPAN, model), bf16),
        in_specs=[spec(hbm)] * 7,
        out_specs=spec(hbm),
        scratch_shapes=[
            vmem(queries.shape, bf16),
            vmem(keys.shape, bf16),
            vmem(values.shape, bf16),
            vmem((128, 2, SPAN, WIDTH), bf16),
            vmem((PIECES, SPAN, GROUP * WIDTH), bf16),
            vmem((PIECES, SPAN, GROUP * WIDTH), bf16),
            vmem(queries.shape, bf16),
            vmem(out_weight.shape, bf16),
            vmem((ROWS, BACK * SPAN), f32),
            vmem((ROWS, BACK * SPAN), f32),
            vmem((ROWS, WIDTH), f32),
            vmem((ROWS, WIDTH), f32),
            vmem((ROWS, WIDTH), f32),
            vmem((ROWS, WIDTH), f32),
            vmem((ROWS, WIDTH), f32),
            vmem((1, BACK * SPAN), i32),
            vmem((PIECES, ROWS, 2 * WIDTH), f32),
            vmem((PIECES, ROWS, WIDTH), f32),
            vmem((PIECES, SPAN, WIDTH), f32),
            vmem((8, 128), i32),
            vmem((count, SPAN, model // count), bf16),
            vmem((count, SPAN, model // count), bf16),
            vmem((count, SPAN, model // count), f32),
            vmem((count, SPAN, model // count), bf16),
            vmem((1, 128), i32),
            vmem((doc_ids.shape[0] // 128, 128), i32),
            pltpu.SMEM((128,), i32),
            pltpu.SMEM((8, 128), i32),
            dma((3,)), dma((3,)), dma, dma, dma((count,)),
            dma((4, 2, 2)), dma((4, 2)), dma((PIECES, 2)), dma((PIECES,)),
            dma((PIECES, 3)), dma((PIECES, 2)), dma((2, 2, PIECES)), dma((3, PIECES)),
            dma((4, 2, PIECES)), dma((4, PIECES)), dma((64,)), dma,
            dma((PIECES,)), dma((PIECES,)), dma((count,)), dma((count,)),
        ],
        compiler_params=pltpu.CompilerParams(
            collective_id=0, has_side_effects=True, vmem_limit_bytes=60 * 2 ** 20,
        ),
    )(span_table, span_table.reshape(1, 128), doc_ids.reshape(-1, 128), queries, keys, values, out_weight)


def solution(mesh):
    return jax.shard_map(
        local,
        mesh=mesh,
        in_specs=(P("cp", "hd"), P("cp", "hd"), P("cp", "hd"), P(), P(), P("hd", None)),
        out_specs=P(("cp", "hd"), None),
        check_vma=False,
    )
```

```python
import functools
import math

import jax
import jax.numpy as jnp
from jax import lax
from jax.experimental import pallas as pl
from jax.experimental.pallas import tpu as pltpu
from jax.sharding import PartitionSpec as P

WIDTH = 128
SPAN = 96
GROUP = 4
ROWS = GROUP * SPAN
PIECES = 8
DOCS = 8
BACK = 32
STEP = 8
KEYS = STEP * SPAN
BLOCKS = BACK * SPAN // 256
NEG = -1e30
MESH = pl.DeviceIdType.MESH
FACTOR = WIDTH ** -0.5 * math.log2(math.e)
ARRIVAL = (0, 1, 3, 4, 2, 5, 7, 6)
EARLY = (2, 5, 7, 6)
LATE = (0, 1, 3, 4)
RETURN = (6, 5, 2, 7, 1, 4, 3, 0)


def kernel(
    span_hbm, span_row_hbm, doc_hbm, q_hbm, k_hbm, v_hbm, w_hbm, out_ref,
    q_in, k_in, v_in, kv, q_buf, o_buf, attn, w_vmem, scores0, scores1, shift0, shift1, fade0, fade1, peak, place_of, own_acc, own_top, penalty, table,
    outgoing, incoming, kept, result_of, span_row_ref, doc_ref, span_ref, index,
    load_sem, small_sem, w_sem, table_sem, out_sem,
    su, sq, ru, rq, s_own, s_far, s_half, s_z, rx, rz, sd, rd, so, ro, xs, xr,
):
    me = lax.axis_index("cp")
    hd = lax.axis_index("hd")
    other = 1 - hd
    x, z, y = me // 16, (me // 4) % 4, me % 4
    home = (z // 2) == hd
    zp = z + 1 - 2 * (z % 2)

    def chip(xx, zz, yy):
        return xx * 16 + zz * 4 + yy

    right, left, across = chip((x + 1) % 4, z, y), chip((x + 3) % 4, z, y), chip(x, zp, y)

    def source(xo, zo, i):
        return chip(xo, 3 - zo if i >= 4 else zo, (y + i % 4) % 4)

    def remote(src, dst, send, recv, cp, core):
        return pltpu.make_async_remote_copy(
            src_ref=src, dst_ref=dst, send_sem=send, recv_sem=recv,
            device_id={"cp": cp, "hd": core}, device_id_type=MESH,
        )

    def landed(dst, sem):
        remote(dst, dst, sd.at[0], sem, me, other).wait_recv()

    def go(copy):
        copy.start()

    def sent(copy):
        copy.wait_send()

    my_rows = pl.ds(pl.multiple_of(hd * SPAN, SPAN), SPAN)
    my_head = pl.ds(pl.multiple_of(y * WIDTH, WIDTH), WIDTH)
    my_queries = pl.ds(pl.multiple_of(y * GROUP * WIDTH, GROUP * WIDTH), GROUP * WIDTH)

    loads = [
        pltpu.make_async_copy(k_hbm, k_in, load_sem.at[0]),
        pltpu.make_async_copy(v_hbm, v_in, load_sem.at[1]),
        pltpu.make_async_copy(q_hbm, q_in, load_sem.at[2]),
    ]
    locals_ = [
        pltpu.make_async_copy(k_hbm.at[my_rows, my_head], kv.at[2 * me + hd, 0], ru.at[0, 0]),
        pltpu.make_async_copy(v_hbm.at[my_rows, my_head], kv.at[2 * me + hd, 1], ru.at[0, 1]),
        pltpu.make_async_copy(q_hbm.at[my_rows, my_queries], q_buf.at[0], rq.at[0]),
    ]
    w_load = pltpu.make_async_copy(w_hbm, w_vmem, w_sem)
    small = [
        pltpu.make_async_copy(span_row_hbm, span_row_ref, small_sem.at[0]),
        pltpu.make_async_copy(doc_hbm, doc_ref, small_sem.at[1]),
        pltpu.make_async_copy(span_hbm, span_ref, small_sem.at[2]),
    ]
    for load in loads + small:
        load.start()

    @pl.when(home)
    def _():
        for copy in locals_:
            copy.start()

    barrier = pltpu.get_barrier_semaphore()

    def greet(cp, core):
        pl.semaphore_signal(barrier, inc=1, device_id={"cp": cp, "hd": core}, device_id_type=MESH)

    for i in range(PIECES):
        for core in (hd, other):
            if i or core is other:
                greet(source(x, z, i), core)
    for target in (right, left, across):
        greet(target, hd)

    for load in small:
        load.wait()
    spans = jnp.broadcast_to(span_row_ref[...].astype(jnp.float32), (128, 128)).T
    held_by = lax.broadcasted_iota(jnp.int32, (128, 128), 0).astype(jnp.float32)
    wanted = lax.broadcasted_iota(jnp.int32, (128, 128), 1).astype(jnp.float32)
    table[0:1, :] = jnp.max(jnp.where(spans == wanted, held_by, 0.0), axis=0, keepdims=True).astype(jnp.int32)
    docs = doc_ref[...]
    lane = lax.broadcasted_iota(jnp.int32, (1, 128), 1)
    starts = jnp.zeros((1, 128), jnp.float32)
    for d in range(1, DOCS):
        first = jnp.sum(jnp.where(docs < d, 1.0, 0.0), keepdims=True)
        starts = jnp.where(lane == d, first, starts)
    table[1:2, :] = starts.astype(jnp.int32)

    pl.semaphore_wait(barrier, 2 * PIECES + 2)

    tz = jnp.where(home, z, 3 - z)

    def scatter(act, what):
        for dj in (0, 1, 3, 2):
            j = (y + dj) % 4
            to = chip(x, tz, j)
            piece = jnp.where(home, 0, 4) + (4 - dj) % 4
            for rel, core in enumerate((hd, other)):
                rows = pl.ds(pl.multiple_of(core * SPAN, SPAN), SPAN)

                def one():
                    if what == "kv":
                        columns = pl.ds(pl.multiple_of(j * WIDTH, WIDTH), WIDTH)
                        for v, staged in enumerate((k_in, v_in)):
                            act(remote(staged.at[rows, columns], kv.at[2 * me + core, v],
                                       su.at[dj, rel, v], ru.at[piece, v], to, core))
                    else:
                        columns = pl.ds(pl.multiple_of(j * GROUP * WIDTH, GROUP * WIDTH), GROUP * WIDTH)
                        act(remote(q_in.at[rows, columns], q_buf.at[piece],
                                   sq.at[dj, rel], rq.at[piece], to, core))

                if dj == 0 and rel == 0:
                    pl.when(jnp.logical_not(home))(one)
                else:
                    one()

    loads[0].wait()
    loads[1].wait()
    scatter(go, "kv")
    loads[2].wait()
    scatter(go, "q")
    w_load.start()
    table_copy = pltpu.make_async_copy(table, index, table_sem)

    def piece_of(xo, zo, i):
        return kv.at[2 * source(xo, zo, i) + hd]

    def share(act, xo, zo, i):
        s = source(xo, zo, i)
        part = kv.at[2 * s + hd]
        act(remote(part, part, sd.at[s], rd, me, other))

    x_left, x_right, x_far = (x + 3) % 4, (x + 1) % 4, (x + 2) % 4

    def relay(act, between=None):
        waiting = act is go
        for i in ARRIVAL:
            part = piece_of(x, z, i)
            if waiting:
                landed(part.at[0], ru.at[i, 0])
                landed(part.at[1], ru.at[i, 1])
            act(remote(part, part, s_own.at[i, 0], rx.at[0, 0, i], right, hd))
            act(remote(part, part, s_own.at[i, 1], rx.at[1, 0, i], left, hd))
            act(remote(part, part, s_own.at[i, 2], rz.at[0, i], across, hd))
            share(act, x, z, i)

        def from_across(i):
            part = piece_of(x, zp, i)
            if waiting:
                landed(part, rz.at[0, i])
            act(remote(part, part, s_far.at[i, 0], rx.at[0, 1, i], right, hd))
            act(remote(part, part, s_far.at[i, 1], rx.at[1, 1, i], left, hd))
            share(act, x, zp, i)

        def from_side(i, zrel, zo):
            for side, xo, onward, half in ((0, x_left, right, 0), (1, x_right, left, 1)):
                part = piece_of(xo, zo, i)
                if waiting:
                    landed(part, rx.at[side, zrel, i])
                act(remote(part.at[half], part.at[half], s_half.at[side, zrel, i],
                           rx.at[2 + side, zrel, i], onward, hd))
                if not zrel and i in LATE:
                    act(remote(part, part, s_z.at[side, i], rz.at[1 + side, i], across, hd))
                share(act, xo, zo, i)

        def from_far(i, zrel, zo):
            part = piece_of(x_far, zo, i)
            if waiting:
                landed(part.at[0], rx.at[2, zrel, i])
                landed(part.at[1], rx.at[3, zrel, i])
            if not zrel and i in LATE:
                act(remote(part, part, s_z.at[2, i], rz.at[3, i], across, hd))
            share(act, x_far, zo, i)

        def last(i, n, xo):
            if waiting:
                landed(piece_of(xo, zp, i), rz.at[n, i])
            share(act, xo, zp, i)

        def extra(k):
            if waiting:
                between(ARRIVAL[k])

        for i in LATE:
            from_side(i, 0, z)
        for i in EARLY:
            from_across(i)
        for i in LATE:
            from_far(i, 0, z)
        for i in EARLY:
            from_side(i, 0, z)
        for k, i in enumerate(EARLY):
            from_side(i, 1, zp)
            extra(k)
        for n, xo in enumerate((x, x_left, x_right)):
            for i in LATE:
                last(i, n, xo)
        for k, i in enumerate(EARLY):
            from_far(i, 0, z)
            extra(k + 4)
        for i in LATE:
            last(i, 3, x_far)
        for i in EARLY:
            from_far(i, 1, zp)

    ones = jnp.ones((KEYS, WIDTH), jnp.bfloat16)

    def slot_of(i):
        return 2 * chip(x, jnp.where(jnp.int32(i) >= 4, 3 - z, z), (y + i % 4) % 4) + hd

    def queries_of(i):
        whole = q_buf[i]
        return jnp.concatenate([whole[:, g * WIDTH:(g + 1) * WIDTH] for g in range(GROUP)], axis=0)

    def score(q, keys):
        return lax.dot_general(q, keys, (((1,), (1,)), ((), ())), preferred_element_type=jnp.float32)

    def own(i):
        landed(q_buf.at[i], rq.at[i])
        slot = slot_of(i)
        begin = span_ref[slot] * SPAN
        row = lax.broadcasted_iota(jnp.int32, (SPAN, WIDTH), 0)
        low = jnp.zeros((SPAN, WIDTH), jnp.int32)
        for d in range(1, DOCS):
            start = index[1, d]
            low = jnp.maximum(low, jnp.where(start <= begin + row, start, 0))
        low = low - begin
        penalty[i] = jnp.where(low < 0, 0.0, -NEG)
        key = lax.broadcasted_iota(jnp.int32, (SPAN, WIDTH), 1)
        bias = jnp.where((key >= low) & (key <= row), 0.0, NEG)[:, :SPAN]
        s = score(queries_of(i), kv[slot, 0]) + jnp.concatenate([bias] * GROUP, axis=0)
        top = jnp.max(s, axis=1, keepdims=True)
        weights = jnp.exp2(s * FACTOR - top * FACTOR).astype(jnp.bfloat16)
        own_top[i] = jnp.broadcast_to(top, (ROWS, WIDTH))
        values = jnp.concatenate([kv[slot, 1], ones[:SPAN]], axis=1)
        own_acc[i] = jnp.dot(weights, values, preferred_element_type=jnp.float32)

    table_copy.start()
    table_copy.wait()
    place = lax.broadcasted_iota(jnp.int32, (1, BACK * SPAN), 1)
    place_of[...] = place - 2 * SPAN * (place // SPAN)
    relay(go, own)

    landed(kv.at[pl.ds(0, 64)], rd)

    def give_back(act, i):
        to = chip(x, jnp.where(i >= 4, 3 - z, z), (y + i % 4) % 4)
        act(remote(o_buf.at[i], attn.at[my_rows, my_queries], so.at[i], ro.at[hd * 4 + y], to, z // 2))

    def slot_at(place):
        return jnp.clip(index[0, jnp.clip(place, 0, 127)], 0, 127)

    def block_of(c, t, which):
        parts = []
        for tile in range(256 * t // SPAN, (256 * t + 255) // SPAN + 1):
            first, last = max(256 * t - SPAN * tile, 0), min(256 * t + 256 - SPAN * tile, SPAN)
            parts.append(kv[slot_at(c - 1 - tile), which, first:last])
        return jnp.concatenate(parts, axis=0)

    def turn(n):
        i = jnp.int32(0)
        for k, piece in enumerate(RETURN):
            i = jnp.where(n == k, piece, i)
        return i

    def stage(ahead, now, before=None):
        if ahead is not None:
            n, s_a, shift_a, fade_a = ahead
            i = turn(n)
            c = span_ref[slot_of(i)]
            begin = c * SPAN
            low = jnp.int32(0)
            for d in range(1, DOCS):
                start = index[1, d]
                low = jnp.maximum(low, jnp.where(start <= begin, start, 0))
            q = queries_of(i)
            reach = low - (begin - SPAN)
            done = 0
        if now is not None:
            nb, s_b, shift_b, fade_b = now
            ib = turn(nb)
            cb = span_ref[slot_of(ib)]
            acc = {}

        def raise_peak(t):
            top = s_a[:, t * KEYS:t * KEYS + WIDTH]
            for l in range(1, KEYS // WIDTH):
                top = jnp.maximum(top, s_a[:, t * KEYS + l * WIDTH:t * KEYS + (l + 1) * WIDTH])
            peak[...] = top if t == 0 else jnp.maximum(peak[...], top)

        for t in range(BLOCKS):
            cut = slice(t * 256, (t + 1) * 256)
            if ahead is not None:
                bias = jnp.where(place_of[:, cut] >= reach, 0.0, NEG)
                s_a[:, cut] = score(q, block_of(c, t, 0)) + bias
                if t >= 4 and (t - 4) % 3 == 0:
                    raise_peak((t - 4) // 3)
            if now is not None:
                shift = shift_b[...]
                shift = jnp.concatenate([shift, shift], axis=1)
                weights = jnp.exp2(s_b[:, cut] * FACTOR - shift).astype(jnp.bfloat16)
                values = jnp.concatenate([block_of(cb, t, 1), ones[:256]], axis=1)
                part = jnp.dot(weights, values, preferred_element_type=jnp.float32)
                chain = 0 if ahead is not None else t % 2
                acc[chain] = acc[chain] + part if chain in acc else part
        if ahead is not None:
            raise_peak(BLOCKS // 3 - 1)
            fence = jnp.concatenate([penalty[i]] * GROUP, axis=0)
            mine = own_top[i]
            top = jnp.maximum(jnp.max(peak[...], axis=1, keepdims=True) - fence, mine)
            fade_a[...] = jnp.exp2((mine - top) * FACTOR)
            shift_a[...] = top * FACTOR + fence
        if now is not None:
            fade = fade_b[...]
            if 1 in acc:
                scores0[:, :2 * WIDTH] = acc[0]
                acc = {0: acc[1] + scores0[:, :2 * WIDTH]}
            acc = acc[0] + own_acc[ib] * jnp.concatenate([fade, fade], axis=1)
            result = (acc[:, :WIDTH] / acc[:, WIDTH:]).astype(jnp.bfloat16)
            for g in range(GROUP):
                o_buf[ib, :, g * WIDTH:(g + 1) * WIDTH] = result[g * SPAN:(g + 1) * SPAN]

    even = (scores0, shift0, fade0)
    odd = (scores1, shift1, fade1)
    stage((jnp.int32(0),) + even, None)
    stage((jnp.int32(1),) + odd, (jnp.int32(0),) + even)
    give_back(go, turn(jnp.int32(0)))

    def pair(k, carry):
        stage((2 * k + 2,) + even, (2 * k + 1,) + odd)
        give_back(go, turn(2 * k + 1))
        stage((2 * k + 3,) + odd, (2 * k + 2,) + even)
        give_back(go, turn(2 * k + 2))
        return carry

    lax.fori_loop(0, PIECES // 2 - 1, pair, 0)
    stage(None, (jnp.int32(PIECES - 1),) + odd)

    @pl.when(home)
    def _():
        attn[my_rows, my_queries] = o_buf[0]

    @pl.when(jnp.logical_not(home))
    def _():
        give_back(go, jnp.int32(0))

    scatter(sent, "kv")
    scatter(sent, "q")
    relay(sent)

    for k in range(2):
        for j in range(4):
            @pl.when(jnp.logical_not(home & (hd == k) & (y == j)))
            def _():
                landed(attn.at[pl.ds(k * SPAN, SPAN), pl.ds(j * GROUP * WIDTH, GROUP * WIDTH)], ro.at[k * 4 + j])

    w_load.wait()
    count, width = outgoing.shape[0], outgoing.shape[2]

    def hand_over(n):
        return remote(outgoing.at[n], incoming.at[n], xs.at[n], xr.at[n], me, other)

    @pl.loop(0, count)
    def _(n):
        columns = pl.ds(pl.multiple_of(n * width, width), width)
        product = jnp.dot(attn[...], w_vmem[:, columns], preferred_element_type=jnp.float32)
        upper, lower = product[:SPAN], product[SPAN:]
        first = hd == 0
        outgoing[n] = jnp.where(first, lower, upper).astype(jnp.bfloat16)
        kept[n] = jnp.where(first, upper, lower)
        hand_over(n).start()

    for i in range(PIECES):
        if i:
            give_back(sent, jnp.int32(i))
        else:
            pl.when(jnp.logical_not(home))(lambda: give_back(sent, jnp.int32(0)))

    def put(n):
        return pltpu.make_async_copy(result_of.at[n], out_ref.at[:, pl.ds(n * width, width)], out_sem.at[n])

    for n in range(count):
        hand_over(n).wait_recv()
        result_of[n] = (kept[n] + incoming[n].astype(jnp.float32)).astype(jnp.bfloat16)
        if n:
            put(n - 1).start()

    put(count - 1).start()
    for n in range(count):
        hand_over(n).wait_send()
        put(n).wait()


def local(queries, keys, values, span_table, doc_ids, out_weight):
    model = out_weight.shape[1]
    count = 8
    vmem, hbm = pltpu.VMEM, pl.ANY
    spec = lambda space: pl.BlockSpec(memory_space=space)
    dma = pltpu.SemaphoreType.DMA
    f32, bf16, i32 = jnp.float32, jnp.bfloat16, jnp.int32
    return pl.pallas_call(
        kernel,
        out_shape=jax.ShapeDtypeStruct((SPAN, model), bf16),
        in_specs=[spec(hbm)] * 7,
        out_specs=spec(hbm),
        scratch_shapes=[
            vmem(queries.shape, bf16),
            vmem(keys.shape, bf16),
            vmem(values.shape, bf16),
            vmem((128, 2, SPAN, WIDTH), bf16),
            vmem((PIECES, SPAN, GROUP * WIDTH), bf16),
            vmem((PIECES, SPAN, GROUP * WIDTH), bf16),
            vmem(queries.shape, bf16),
            vmem(out_weight.shape, bf16),
            vmem((ROWS, BACK * SPAN), f32),
            vmem((ROWS, BACK * SPAN), f32),
            vmem((ROWS, WIDTH), f32),
            vmem((ROWS, WIDTH), f32),
            vmem((ROWS, WIDTH), f32),
            vmem((ROWS, WIDTH), f32),
            vmem((ROWS, WIDTH), f32),
            vmem((1, BACK * SPAN), i32),
            vmem((PIECES, ROWS, 2 * WIDTH), f32),
            vmem((PIECES, ROWS, WIDTH), f32),
            vmem((PIECES, SPAN, WIDTH), f32),
            vmem((8, 128), i32),
            vmem((count, SPAN, model // count), bf16),
            vmem((count, SPAN, model // count), bf16),
            vmem((count, SPAN, model // count), f32),
            vmem((count, SPAN, model // count), bf16),
            vmem((1, 128), i32),
            vmem((doc_ids.shape[0] // 128, 128), i32),
            pltpu.SMEM((128,), i32),
            pltpu.SMEM((8, 128), i32),
            dma((3,)), dma((3,)), dma, dma, dma((count,)),
            dma((4, 2, 2)), dma((4, 2)), dma((PIECES, 2)), dma((PIECES,)),
            dma((PIECES, 3)), dma((PIECES, 2)), dma((2, 2, PIECES)), dma((3, PIECES)),
            dma((4, 2, PIECES)), dma((4, PIECES)), dma((64,)), dma,
            dma((PIECES,)), dma((PIECES,)), dma((count,)), dma((count,)),
        ],
        compiler_params=pltpu.CompilerParams(
            collective_id=0, has_side_effects=True, vmem_limit_bytes=60 * 2 ** 20,
        ),
    )(span_table, span_table.reshape(1, 128), doc_ids.reshape(-1, 128), queries, keys, values, out_weight)


def solution(mesh):
    return jax.shard_map(
        local,
        mesh=mesh,
        in_specs=(P("cp", "hd"), P("cp", "hd"), P("cp", "hd"), P(), P(), P("hd", None)),
        out_specs=P(("cp", "hd"), None),
        check_vma=False,
    )
```

```python
import functools
import math

import jax
import jax.numpy as jnp
from jax import lax
from jax.experimental import pallas as pl
from jax.experimental.pallas import tpu as pltpu
from jax.sharding import PartitionSpec as P

WIDTH = 128
SPAN = 96
GROUP = 4
ROWS = GROUP * SPAN
PIECES = 8
DOCS = 8
BACK = 32
STEP = 8
KEYS = STEP * SPAN
BLOCKS = BACK * SPAN // 256
NEG = -1e30
MESH = pl.DeviceIdType.MESH
FACTOR = WIDTH ** -0.5 * math.log2(math.e)
ARRIVAL = (0, 1, 3, 4, 2, 5, 7, 6)
EARLY = (2, 5, 7, 6)
LATE = (0, 1, 3, 4)
RETURN = (6, 5, 2, 7, 1, 4, 3, 0)


def kernel(
    span_hbm, span_row_hbm, doc_hbm, q_hbm, k_hbm, v_hbm, w_hbm, out_ref,
    q_in, k_in, v_in, kv, q_buf, o_buf, attn, w_vmem, scores0, scores1, shift0, shift1, fade0, fade1, peak, place_of, own_acc, own_top, penalty, table,
    outgoing, incoming, kept, result_of, span_row_ref, doc_ref, span_ref, index,
    load_sem, small_sem, w_sem, table_sem, out_sem,
    su, sq, ru, rq, s_own, s_far, s_half, s_z, rx, rz, sd, rd, so, ro, xs, xr,
):
    me = lax.axis_index("cp")
    hd = lax.axis_index("hd")
    other = 1 - hd
    x, z, y = me // 16, (me // 4) % 4, me % 4
    home = (z // 2) == hd
    zp = z + 1 - 2 * (z % 2)

    def chip(xx, zz, yy):
        return xx * 16 + zz * 4 + yy

    right, left, across = chip((x + 1) % 4, z, y), chip((x + 3) % 4, z, y), chip(x, zp, y)

    def source(xo, zo, i):
        return chip(xo, 3 - zo if i >= 4 else zo, (y + i % 4) % 4)

    def remote(src, dst, send, recv, cp, core):
        return pltpu.make_async_remote_copy(
            src_ref=src, dst_ref=dst, send_sem=send, recv_sem=recv,
            device_id={"cp": cp, "hd": core}, device_id_type=MESH,
        )

    def landed(dst, sem):
        remote(dst, dst, sd.at[0], sem, me, other).wait_recv()

    def go(copy):
        copy.start()

    def sent(copy):
        copy.wait_send()

    my_rows = pl.ds(pl.multiple_of(hd * SPAN, SPAN), SPAN)
    my_head = pl.ds(pl.multiple_of(y * WIDTH, WIDTH), WIDTH)
    my_queries = pl.ds(pl.multiple_of(y * GROUP * WIDTH, GROUP * WIDTH), GROUP * WIDTH)

    loads = [
        pltpu.make_async_copy(k_hbm, k_in, load_sem.at[0]),
        pltpu.make_async_copy(v_hbm, v_in, load_sem.at[1]),
        pltpu.make_async_copy(q_hbm, q_in, load_sem.at[2]),
    ]
    locals_ = [
        pltpu.make_async_copy(k_hbm.at[my_rows, my_head], kv.at[2 * me + hd, 0], ru.at[0, 0]),
        pltpu.make_async_copy(v_hbm.at[my_rows, my_head], kv.at[2 * me + hd, 1], ru.at[0, 1]),
        pltpu.make_async_copy(q_hbm.at[my_rows, my_queries], q_buf.at[0], rq.at[0]),
    ]
    w_load = pltpu.make_async_copy(w_hbm, w_vmem, w_sem)
    small = [
        pltpu.make_async_copy(span_row_hbm, span_row_ref, small_sem.at[0]),
        pltpu.make_async_copy(doc_hbm, doc_ref, small_sem.at[1]),
        pltpu.make_async_copy(span_hbm, span_ref, small_sem.at[2]),
    ]
    for load in loads + small:
        load.start()

    @pl.when(home)
    def _():
        for copy in locals_:
            copy.start()

    barrier = pltpu.get_barrier_semaphore()

    def greet(cp, core):
        pl.semaphore_signal(barrier, inc=1, device_id={"cp": cp, "hd": core}, device_id_type=MESH)

    for i in range(PIECES):
        for core in (hd, other):
            if i or core is other:
                greet(source(x, z, i), core)
    for target in (right, left, across):
        greet(target, hd)

    for load in small:
        load.wait()
    spans = jnp.broadcast_to(span_row_ref[...].astype(jnp.float32), (128, 128)).T
    held_by = lax.broadcasted_iota(jnp.int32, (128, 128), 0).astype(jnp.float32)
    wanted = lax.broadcasted_iota(jnp.int32, (128, 128), 1).astype(jnp.float32)
    table[0:1, :] = jnp.max(jnp.where(spans == wanted, held_by, 0.0), axis=0, keepdims=True).astype(jnp.int32)
    docs = doc_ref[...]
    lane = lax.broadcasted_iota(jnp.int32, (1, 128), 1)
    starts = jnp.zeros((1, 128), jnp.float32)
    for d in range(1, DOCS):
        first = jnp.sum(jnp.where(docs < d, 1.0, 0.0), keepdims=True)
        starts = jnp.where(lane == d, first, starts)
    table[1:2, :] = starts.astype(jnp.int32)

    pl.semaphore_wait(barrier, 2 * PIECES + 2)

    tz = jnp.where(home, z, 3 - z)

    def scatter(act, what):
        for dj in (0, 1, 3, 2):
            j = (y + dj) % 4
            to = chip(x, tz, j)
            piece = jnp.where(home, 0, 4) + (4 - dj) % 4
            for rel, core in enumerate((hd, other)):
                rows = pl.ds(pl.multiple_of(core * SPAN, SPAN), SPAN)

                def one():
                    if what == "kv":
                        columns = pl.ds(pl.multiple_of(j * WIDTH, WIDTH), WIDTH)
                        for v, staged in enumerate((k_in, v_in)):
                            act(remote(staged.at[rows, columns], kv.at[2 * me + core, v],
                                       su.at[dj, rel, v], ru.at[piece, v], to, core))
                    else:
                        columns = pl.ds(pl.multiple_of(j * GROUP * WIDTH, GROUP * WIDTH), GROUP * WIDTH)
                        act(remote(q_in.at[rows, columns], q_buf.at[piece],
                                   sq.at[dj, rel], rq.at[piece], to, core))

                if dj == 0 and rel == 0:
                    pl.when(jnp.logical_not(home))(one)
                else:
                    one()

    loads[0].wait()
    loads[1].wait()
    scatter(go, "kv")
    loads[2].wait()
    scatter(go, "q")
    w_load.start()
    table_copy = pltpu.make_async_copy(table, index, table_sem)

    def piece_of(xo, zo, i):
        return kv.at[2 * source(xo, zo, i) + hd]

    def share(act, xo, zo, i):
        s = source(xo, zo, i)
        part = kv.at[2 * s + hd]
        act(remote(part, part, sd.at[s], rd, me, other))

    x_left, x_right, x_far = (x + 3) % 4, (x + 1) % 4, (x + 2) % 4

    def relay(act, between=None):
        waiting = act is go
        for i in ARRIVAL:
            part = piece_of(x, z, i)
            if waiting:
                landed(part.at[0], ru.at[i, 0])
                landed(part.at[1], ru.at[i, 1])
            act(remote(part, part, s_own.at[i, 0], rx.at[0, 0, i], right, hd))
            act(remote(part, part, s_own.at[i, 1], rx.at[1, 0, i], left, hd))
            act(remote(part, part, s_own.at[i, 2], rz.at[0, i], across, hd))
            share(act, x, z, i)

        def from_across(i):
            part = piece_of(x, zp, i)
            if waiting:
                landed(part, rz.at[0, i])
            act(remote(part, part, s_far.at[i, 0], rx.at[0, 1, i], right, hd))
            act(remote(part, part, s_far.at[i, 1], rx.at[1, 1, i], left, hd))
            share(act, x, zp, i)

        def from_side(i, zrel, zo):
            for side, xo, onward, half in ((0, x_left, right, 0), (1, x_right, left, 1)):
                part = piece_of(xo, zo, i)
                if waiting:
                    landed(part, rx.at[side, zrel, i])
                act(remote(part.at[half], part.at[half], s_half.at[side, zrel, i],
                           rx.at[2 + side, zrel, i], onward, hd))
                if not zrel and i in LATE:
                    act(remote(part, part, s_z.at[side, i], rz.at[1 + side, i], across, hd))
                share(act, xo, zo, i)

        def from_far(i, zrel, zo):
            part = piece_of(x_far, zo, i)
            if waiting:
                landed(part.at[0], rx.at[2, zrel, i])
                landed(part.at[1], rx.at[3, zrel, i])
            if not zrel and i in LATE:
                act(remote(part, part, s_z.at[2, i], rz.at[3, i], across, hd))
            share(act, x_far, zo, i)

        def last(i, n, xo):
            if waiting:
                landed(piece_of(xo, zp, i), rz.at[n, i])
            share(act, xo, zp, i)

        def extra(k):
            if waiting:
                between(ARRIVAL[k])

        for i in LATE:
            from_side(i, 0, z)
        for i in EARLY:
            from_across(i)
        for i in LATE:
            last(i, 0, x)
        for i in LATE:
            from_far(i, 0, z)
        for i in EARLY:
            from_side(i, 0, z)
        for k, i in enumerate(EARLY):
            from_side(i, 1, zp)
            extra(k)
        for n, xo in ((1, x_left), (2, x_right)):
            for i in LATE:
                last(i, n, xo)
        for k, i in enumerate(EARLY):
            from_far(i, 0, z)
            extra(k + 4)
        for i in LATE:
            last(i, 3, x_far)
        for i in EARLY:
            from_far(i, 1, zp)

    ones = jnp.ones((KEYS, WIDTH), jnp.bfloat16)

    def slot_of(i):
        return 2 * chip(x, jnp.where(jnp.int32(i) >= 4, 3 - z, z), (y + i % 4) % 4) + hd

    def queries_of(i):
        whole = q_buf[i]
        return jnp.concatenate([whole[:, g * WIDTH:(g + 1) * WIDTH] for g in range(GROUP)], axis=0)

    def score(q, keys):
        return lax.dot_general(q, keys, (((1,), (1,)), ((), ())), preferred_element_type=jnp.float32)

    def own(i):
        landed(q_buf.at[i], rq.at[i])
        slot = slot_of(i)
        begin = span_ref[slot] * SPAN
        row = lax.broadcasted_iota(jnp.int32, (SPAN, WIDTH), 0)
        low = jnp.zeros((SPAN, WIDTH), jnp.int32)
        for d in range(1, DOCS):
            start = index[1, d]
            low = jnp.maximum(low, jnp.where(start <= begin + row, start, 0))
        low = low - begin
        penalty[i] = jnp.where(low < 0, 0.0, -NEG)
        key = lax.broadcasted_iota(jnp.int32, (SPAN, WIDTH), 1)
        bias = jnp.where((key >= low) & (key <= row), 0.0, NEG)[:, :SPAN]
        s = score(queries_of(i), kv[slot, 0]) + jnp.concatenate([bias] * GROUP, axis=0)
        top = jnp.max(s, axis=1, keepdims=True)
        weights = jnp.exp2(s * FACTOR - top * FACTOR).astype(jnp.bfloat16)
        own_top[i] = jnp.broadcast_to(top, (ROWS, WIDTH))
        values = jnp.concatenate([kv[slot, 1], ones[:SPAN]], axis=1)
        own_acc[i] = jnp.dot(weights, values, preferred_element_type=jnp.float32)

    table_copy.start()
    table_copy.wait()
    place = lax.broadcasted_iota(jnp.int32, (1, BACK * SPAN), 1)
    place_of[...] = place - 2 * SPAN * (place // SPAN)
    relay(go, own)

    landed(kv.at[pl.ds(0, 64)], rd)

    def give_back(act, i):
        to = chip(x, jnp.where(i >= 4, 3 - z, z), (y + i % 4) % 4)
        act(remote(o_buf.at[i], attn.at[my_rows, my_queries], so.at[i], ro.at[hd * 4 + y], to, z // 2))

    def slot_at(place):
        return jnp.clip(index[0, jnp.clip(place, 0, 127)], 0, 127)

    def block_of(c, t, which):
        parts = []
        for tile in range(256 * t // SPAN, (256 * t + 255) // SPAN + 1):
            first, last = max(256 * t - SPAN * tile, 0), min(256 * t + 256 - SPAN * tile, SPAN)
            parts.append(kv[slot_at(c - 1 - tile), which, first:last])
        return jnp.concatenate(parts, axis=0)

    def turn(n):
        i = jnp.int32(0)
        for k, piece in enumerate(RETURN):
            i = jnp.where(n == k, piece, i)
        return i

    def stage(ahead, now, before=None):
        if ahead is not None:
            n, s_a, shift_a, fade_a = ahead
            i = turn(n)
            c = span_ref[slot_of(i)]
            begin = c * SPAN
            low = jnp.int32(0)
            for d in range(1, DOCS):
                start = index[1, d]
                low = jnp.maximum(low, jnp.where(start <= begin, start, 0))
            q = queries_of(i)
            reach = low - (begin - SPAN)
            done = 0
        if now is not None:
            nb, s_b, shift_b, fade_b = now
            ib = turn(nb)
            cb = span_ref[slot_of(ib)]
            acc = {}

        def raise_peak(t):
            top = s_a[:, t * KEYS:t * KEYS + WIDTH]
            for l in range(1, KEYS // WIDTH):
                top = jnp.maximum(top, s_a[:, t * KEYS + l * WIDTH:t * KEYS + (l + 1) * WIDTH])
            peak[...] = top if t == 0 else jnp.maximum(peak[...], top)

        for t in range(BLOCKS):
            cut = slice(t * 256, (t + 1) * 256)
            if ahead is not None:
                bias = jnp.where(place_of[:, cut] >= reach, 0.0, NEG)
                s_a[:, cut] = score(q, block_of(c, t, 0)) + bias
                if t >= 4 and (t - 4) % 3 == 0:
                    raise_peak((t - 4) // 3)
            if now is not None:
                shift = shift_b[...]
                shift = jnp.concatenate([shift, shift], axis=1)
                weights = jnp.exp2(s_b[:, cut] * FACTOR - shift).astype(jnp.bfloat16)
                values = jnp.concatenate([block_of(cb, t, 1), ones[:256]], axis=1)
                part = jnp.dot(weights, values, preferred_element_type=jnp.float32)
                chain = 0 if ahead is not None else t % 2
                acc[chain] = acc[chain] + part if chain in acc else part
        if ahead is not None:
            raise_peak(BLOCKS // 3 - 1)
            fence = jnp.concatenate([penalty[i]] * GROUP, axis=0)
            mine = own_top[i]
            top = jnp.maximum(jnp.max(peak[...], axis=1, keepdims=True) - fence, mine)
            fade_a[...] = jnp.exp2((mine - top) * FACTOR)
            shift_a[...] = top * FACTOR + fence
        if now is not None:
            fade = fade_b[...]
            if 1 in acc:
                scores0[:, :2 * WIDTH] = acc[0]
                acc = {0: acc[1] + scores0[:, :2 * WIDTH]}
            acc = acc[0] + own_acc[ib] * jnp.concatenate([fade, fade], axis=1)
            result = (acc[:, :WIDTH] / acc[:, WIDTH:]).astype(jnp.bfloat16)
            for g in range(GROUP):
                o_buf[ib, :, g * WIDTH:(g + 1) * WIDTH] = result[g * SPAN:(g + 1) * SPAN]

    even = (scores0, shift0, fade0)
    odd = (scores1, shift1, fade1)
    stage((jnp.int32(0),) + even, None)
    stage((jnp.int32(1),) + odd, (jnp.int32(0),) + even)
    give_back(go, turn(jnp.int32(0)))

    def pair(k, carry):
        stage((2 * k + 2,) + even, (2 * k + 1,) + odd)
        give_back(go, turn(2 * k + 1))
        stage((2 * k + 3,) + odd, (2 * k + 2,) + even)
        give_back(go, turn(2 * k + 2))
        return carry

    lax.fori_loop(0, PIECES // 2 - 1, pair, 0)
    stage(None, (jnp.int32(PIECES - 1),) + odd)

    @pl.when(home)
    def _():
        attn[my_rows, my_queries] = o_buf[0]

    @pl.when(jnp.logical_not(home))
    def _():
        give_back(go, jnp.int32(0))

    scatter(sent, "kv")
    scatter(sent, "q")
    relay(sent)

    for k in range(2):
        for j in range(4):
            @pl.when(jnp.logical_not(home & (hd == k) & (y == j)))
            def _():
                landed(attn.at[pl.ds(k * SPAN, SPAN), pl.ds(j * GROUP * WIDTH, GROUP * WIDTH)], ro.at[k * 4 + j])

    w_load.wait()
    count, width = outgoing.shape[0], outgoing.shape[2]

    def hand_over(n):
        return remote(outgoing.at[n], incoming.at[n], xs.at[n], xr.at[n], me, other)

    @pl.loop(0, count)
    def _(n):
        columns = pl.ds(pl.multiple_of(n * width, width), width)
        product = jnp.dot(attn[...], w_vmem[:, columns], preferred_element_type=jnp.float32)
        upper, lower = product[:SPAN], product[SPAN:]
        first = hd == 0
        outgoing[n] = jnp.where(first, lower, upper).astype(jnp.bfloat16)
        kept[n] = jnp.where(first, upper, lower)
        hand_over(n).start()

    for i in range(PIECES):
        if i:
            give_back(sent, jnp.int32(i))
        else:
            pl.when(jnp.logical_not(home))(lambda: give_back(sent, jnp.int32(0)))

    def put(n):
        return pltpu.make_async_copy(result_of.at[n], out_ref.at[:, pl.ds(n * width, width)], out_sem.at[n])

    for n in range(count):
        hand_over(n).wait_recv()
        result_of[n] = (kept[n] + incoming[n].astype(jnp.float32)).astype(jnp.bfloat16)
        if n:
            put(n - 1).start()

    put(count - 1).start()
    for n in range(count):
        hand_over(n).wait_send()
        put(n).wait()


def local(queries, keys, values, span_table, doc_ids, out_weight):
    model = out_weight.shape[1]
    count = 8
    vmem, hbm = pltpu.VMEM, pl.ANY
    spec = lambda space: pl.BlockSpec(memory_space=space)
    dma = pltpu.SemaphoreType.DMA
    f32, bf16, i32 = jnp.float32, jnp.bfloat16, jnp.int32
    return pl.pallas_call(
        kernel,
        out_shape=jax.ShapeDtypeStruct((SPAN, model), bf16),
        in_specs=[spec(hbm)] * 7,
        out_specs=spec(hbm),
        scratch_shapes=[
            vmem(queries.shape, bf16),
            vmem(keys.shape, bf16),
            vmem(values.shape, bf16),
            vmem((128, 2, SPAN, WIDTH), bf16),
            vmem((PIECES, SPAN, GROUP * WIDTH), bf16),
            vmem((PIECES, SPAN, GROUP * WIDTH), bf16),
            vmem(queries.shape, bf16),
            vmem(out_weight.shape, bf16),
            vmem((ROWS, BACK * SPAN), f32),
            vmem((ROWS, BACK * SPAN), f32),
            vmem((ROWS, WIDTH), f32),
            vmem((ROWS, WIDTH), f32),
            vmem((ROWS, WIDTH), f32),
            vmem((ROWS, WIDTH), f32),
            vmem((ROWS, WIDTH), f32),
            vmem((1, BACK * SPAN), i32),
            vmem((PIECES, ROWS, 2 * WIDTH), f32),
            vmem((PIECES, ROWS, WIDTH), f32),
            vmem((PIECES, SPAN, WIDTH), f32),
            vmem((8, 128), i32),
            vmem((count, SPAN, model // count), bf16),
            vmem((count, SPAN, model // count), bf16),
            vmem((count, SPAN, model // count), f32),
            vmem((count, SPAN, model // count), bf16),
            vmem((1, 128), i32),
            vmem((doc_ids.shape[0] // 128, 128), i32),
            pltpu.SMEM((128,), i32),
            pltpu.SMEM((8, 128), i32),
            dma((3,)), dma((3,)), dma, dma, dma((count,)),
            dma((4, 2, 2)), dma((4, 2)), dma((PIECES, 2)), dma((PIECES,)),
            dma((PIECES, 3)), dma((PIECES, 2)), dma((2, 2, PIECES)), dma((3, PIECES)),
            dma((4, 2, PIECES)), dma((4, PIECES)), dma((64,)), dma,
            dma((PIECES,)), dma((PIECES,)), dma((count,)), dma((count,)),
        ],
        compiler_params=pltpu.CompilerParams(
            collective_id=0, has_side_effects=True, vmem_limit_bytes=60 * 2 ** 20,
        ),
    )(span_table, span_table.reshape(1, 128), doc_ids.reshape(-1, 128), queries, keys, values, out_weight)


def solution(mesh):
    return jax.shard_map(
        local,
        mesh=mesh,
        in_specs=(P("cp", "hd"), P("cp", "hd"), P("cp", "hd"), P(), P(), P("hd", None)),
        out_specs=P(("cp", "hd"), None),
        check_vma=False,
    )
```
